128 devices in a mesh: ga: 16 (over x, z_hi, core), ba: 8 (over y, z_lo).
Axes of the slice: x: 4, y: 4, z: 4 (z_hi: 2, z_lo: 2; z = z_hi * 2 + z_lo), core: 2. Of those that a mesh axis runs over, the one named last changes fastest.
Arguments:
- psi: float32 [2, 32768, 2048], P(None, 'ga', 'ba'), may hold values from -0.15625 to 0.15625
- dpsi: float32 [2, 32768, 512], P(None, 'ga', 'ba'), may hold values from -6 to 6
- band_weight: float32 [2048], replicated, may hold values from 0.25 to 1
- panel_band: int32 [16], P('ba'), may hold values from 0 to 15, each once
- slab_offset: int32 [16], replicated, may hold values from 0 to 2047
Outputs:
- projected: float32 [2, 32768, 512], P(None, 'ga', 'ba')
The draws below stay inside these ranges and needn't reach their ends.
Inputs may be any that keep to these rules, and one draw needn't show every extreme that they name: panel_band is a permutation of the panel numbers.
All inputs are finite; a program needn't handle non-finite values.
Results may differ from the reference program's by a relative error of at most 0.00012.
Values sent between devices are 32-bit elements; how exact they have to be, the bound alone decides.
A program may use at most 128 MiB of HBM per device.

```python
import math
import jax
import jax.numpy as jnp
from jax import lax

NB = 2048
NP = 512
PANEL = 128
NPW_DEV = 2048
NPW = 32768
NPANEL = 16
N_GA = 16


def place_ends(array, rng, low, high):
    place = [jax.random.randint(jax.random.fold_in(rng, axis), (), 0, length) for axis, length in enumerate(array.shape)]
    widest = array.shape.index(max(array.shape))
    neighbour = place[:widest] + [(place[widest] + 1) % array.shape[widest]] + place[widest + 1:]
    return array.at[tuple(place)].set(low).at[tuple(neighbour)].set(high)


def block_scale(rng, shape, shards, least, top_value):
    def one(position, shards_of):
        steps = jax.random.uniform(jax.random.fold_in(jax.random.fold_in(rng, 6), position), (shards_of,), jnp.float32, least / len(shards), top_value / len(shards))
        return jnp.repeat(jnp.exp(steps), shape[position] // shards_of).reshape((-1,) + (1,) * (len(shape) - position - 1))

    factor_of = one(*shards[0])
    for cut in shards[1:]:
        factor_of = factor_of * one(*cut)
    return factor_of


def scatter_about(key, extent, deviation, reach, shards=(), held_as=jnp.bfloat16):
    drawn = jax.random.normal(key, extent, jnp.float32) * deviation
    if len(shards) > 0:
        drawn = block_scale(key, extent, shards, -0.22, 0.18) * drawn
    return jnp.clip(drawn, min=-reach, max=reach).astype(held_as)


def setup_inputs(seed: int = 0) -> dict:
    seeds = jax.random.split(jax.random.key(seed), 6)
    return {
        "psi": scatter_about(seeds[0], (2, NPW, NB), ((NPW * NB) ** -0.25), 0.15625, ((1, 16), (2, 8)), jnp.float32),
        "dpsi": scatter_about(seeds[1], (2, NPW, NP), 1.0, 6.0, ((1, 16), (2, 8)), jnp.float32),
        "band_weight": jnp.clip(jnp.exp(jax.random.uniform(seeds[2], (NB,), jnp.float32, math.log(0.25), math.log(1.0))), 0.25, 1.0),
        "panel_band": jax.random.permutation(seeds[3], NPANEL).astype(jnp.int32),
        "slab_offset": place_ends(jax.random.randint(seeds[4], (N_GA,), 0, NPW_DEV), jax.random.fold_in(seeds[4], 1), 0, NPW_DEV - 1).astype(jnp.int32),
    }


def tdot(left, right):
    return lax.dot_general(left, right, (((0,), (0,)), ((), ())), precision=lax.Precision.HIGHEST, preferred_element_type=jnp.float32)


def mdot(left, right):
    return jnp.dot(left, right, precision=lax.Precision.HIGHEST, preferred_element_type=jnp.float32)


def reference(psi, dpsi, band_weight, panel_band, slab_offset):
    stacked = dpsi.reshape(2, N_GA, NPW_DEV, NP)
    rows = (jnp.arange(NPW_DEV, dtype=jnp.int32)[None, :] + slab_offset[:, None]) % NPW_DEV
    aligned = jnp.take_along_axis(stacked, rows[None, :, :, None], axis=2).reshape(2, NPW, NP)
    weight = band_weight.reshape(NPANEL, PANEL)[panel_band].reshape(NB)
    over_re = tdot(psi[0], aligned[0]) + tdot(psi[1], aligned[1])
    over_im = tdot(psi[0], aligned[1]) - tdot(psi[1], aligned[0])
    w_re = over_re * weight[:, None]
    w_im = over_im * weight[:, None]
    corr_re = mdot(psi[0], w_re) - mdot(psi[1], w_im)
    corr_im = mdot(psi[0], w_im) + mdot(psi[1], w_re)
    diff = (aligned - jnp.stack([corr_re, corr_im])).reshape(2, N_GA, NPW_DEV, NP)
    back = (jnp.arange(NPW_DEV, dtype=jnp.int32)[None, :] - slab_offset[:, None]) % NPW_DEV
    result = jnp.take_along_axis(diff, back[None, :, :, None], axis=2)
    return result.reshape(2, NPW, NP)
```

```python
import jax
import jax.numpy as jnp
from jax import lax
from jax.experimental import pallas as pl
from jax.experimental.pallas import tpu as pltpu
from jax.sharding import PartitionSpec as P

F32, BF16 = jnp.float32, jnp.bfloat16
PANEL = 128
SLAB = 2048
HALF = SLAB // 2
BANDS = 256
COLS = 128
CHUNK = 256
NC = HALF // CHUNK
NT = (((1,), (1,)), ((), ()))


def split(value):
    high = value.astype(BF16)
    return high, (value - high.astype(F32)).astype(BF16)


def three(dot, left, right):
    return dot(left[0], right[0]) + (dot(left[0], right[1]) + dot(left[1], right[0]))


def nn(left, right):
    return jnp.dot(left, right, preferred_element_type=F32)


def nt(left, right):
    return lax.dot_general(left, right, NT, preferred_element_type=F32)


def kernel(
    at, psi, wt, out,
    psi_o, psi_p, a_v, a_hi, a_lo, p_hi, p_lo, wv, m, w, c,
    r0, r1, r2, s, rl, fin, zin,
    local_sem, a_s, a_r, p_s, p_r, g_s, g_r, c_s, c_r,
):
    ga, ba = lax.axis_index("ga"), lax.axis_index("ba")
    x, zhi, core = ga // 4, (ga // 2) % 2, ga % 2
    y, o = ba // 2, ba % 2
    p = 1 - o
    z = zhi * 2 + o
    oc = 1 - core

    def device(x=x, z=z, y=y, core=core):
        return (x * 4 + (z // 2) * 2 + core, y * 2 + z % 2)

    pair = device(z=zhi * 2 + p)
    up, down = device(y=(y + 1) % 4), device(y=(y + 3) % 4)
    other = device(core=oc)
    along_x = [device(x=(x + k) % 4) for k in (1, 2, 3)]
    along_z = [device(z=(z + k) % 4) for k in (1, 2, 3)]

    sent = []

    def send(src, dst, sems, index, to):
        copy = pltpu.make_async_remote_copy(
            src_ref=src, dst_ref=dst, send_sem=sems[0].at[index], recv_sem=sems[1].at[index],
            device_id=to, device_id_type=pl.DeviceIdType.MESH,
        )
        copy.start()
        sent.append(copy)
        return copy

    local = pltpu.make_async_copy(
        psi.at[:, pl.ds(pl.multiple_of(o * HALF, HALF), HALF), :], psi_o, local_sem
    )
    local.start()

    barrier = pltpu.get_barrier_semaphore()
    peers = [up, down, other, *along_x, *along_z]
    for peer in peers:
        pl.semaphore_signal(barrier, inc=1, device_id=peer, device_id_type=pl.DeviceIdType.MESH)
    pl.semaphore_wait(barrier, len(peers))

    A = (a_s, a_r)
    mine = at.at[:, pl.ds(pl.multiple_of(o * HALF, HALF), HALF)]
    theirs = at.at[:, pl.ds(pl.multiple_of(p * HALF, HALF), HALF)]
    a_pair = send(theirs, a_v.at[3, o], A, 0, pair)
    w_pair = send(wt, wv.at[o], A, 7, pair)
    a_up_o = send(mine, a_v.at[2, o], A, 1, up)
    a_down_o = send(mine, a_v.at[1, o], A, 2, down)
    waves = [
        send(
            psi.at[:, pl.ds(pl.multiple_of(p * HALF + k * CHUNK, CHUNK), CHUNK), :],
            psi_p.at[:, pl.ds(k * CHUNK, CHUNK), :], (p_s, p_r), k, pair,
        )
        for k in range(NC)
    ]

    def keep_columns(value, rel, half):
        rows = rel * 256 + half * COLS
        top = pl.ds(pl.multiple_of(rows, 64), 64)
        bottom = pl.ds(pl.multiple_of(rows + 64, 64), 64)
        for ref, part in zip((a_hi, a_lo), split(value)):
            ref[top, :HALF] = part[:64]
            ref[bottom, :HALF] = part[64:]
            ref[top, HALF:] = part[64:]
            ref[bottom, HALF:] = -part[:64]

    def keep_waves(ref, half, first, count):
        def body(k, _):
            rows = pl.ds(pl.multiple_of(first + k * CHUNK, CHUNK), CHUNK)
            for part in (0, 1):
                high, low = split(ref[part, rows, :])
                at_rows = pl.ds(pl.multiple_of(part * HALF + first + k * CHUNK, CHUNK), CHUNK)
                p_hi[half, at_rows, :] = high
                p_lo[half, at_rows, :] = low
            return 0

        lax.fori_loop(0, count, body, 0)

    wv[o] = wt[...]
    keep_columns(at[:, pl.ds(pl.multiple_of(o * HALF, HALF), HALF)], 3, o)
    local.wait()
    keep_waves(psi_o, o, 0, NC)

    a_pair.wait_recv()
    a_up_p = send(a_v.at[3, p], a_v.at[2, p], A, 3, up)
    a_down_p = send(a_v.at[3, p], a_v.at[1, p], A, 4, down)
    a_up_o.wait_recv()
    far_o = send(a_v.at[2, o], a_v.at[0, o], A, 5, up)
    keep_columns(a_v[3, p], 3, p)
    keep_columns(a_v[2, o], 2, o)
    a_down_o.wait_recv()
    keep_columns(a_v[1, o], 1, o)
    a_down_p.wait_recv()
    far_p = send(a_v.at[1, p], a_v.at[0, p], A, 6, down)
    keep_columns(a_v[1, p], 1, p)
    a_up_p.wait_recv()
    keep_columns(a_v[2, p], 2, p)
    waves[0].wait_recv()
    keep_waves(psi_p, p, 0, 1)
    far_o.wait_recv()
    keep_columns(a_v[0, o], 0, o)
    far_p.wait_recv()
    keep_columns(a_v[0, p], 0, p)
    w_pair.wait_recv()

    def own_bands(rel, _):
        rows = pl.ds(pl.multiple_of(rel * 256, 256), 256)
        left = (a_hi[rows, :], a_lo[rows, :])
        m[o, rows, :] = three(nn, left, (p_hi[o], p_lo[o]))
        return 0

    lax.fori_loop(0, 4, own_bands, 0)

    def pair_bands(rel, k):
        rows = pl.ds(rel * 256, 256) if isinstance(rel, int) else pl.ds(pl.multiple_of(rel * 256, 256), 256)
        total = None if k == 0 else m[p, rows, :]
        for first in (k * CHUNK, HALF + k * CHUNK):
            ks = pl.ds(first, CHUNK)
            term = three(
                nn, (a_hi[rows, ks], a_lo[rows, ks]), (p_hi[p, ks, :], p_lo[p, ks, :])
            )
            total = term if total is None else total + term
        m[p, rows, :] = total

    def pair_bands_all(k):
        def body(rel, _):
            pair_bands(rel, k)
            return 0

        lax.fori_loop(0, 4, body, 0)

    pair_bands_all(0)
    for k in range(1, NC):
        waves[k].wait_recv()
        keep_waves(psi_p, p, k * CHUNK, 1)
        if k < NC - 1:
            pair_bands_all(k)

    G = (g_s, g_r)
    flight = {}

    def rows_of(rel, who, length, first=0):
        return pl.ds(pl.multiple_of(rel * 256 + first + who * length, 16), length)

    def lanes_of(q):
        return pl.ds(pl.multiple_of((q % 2) * 128, 128), 128)

    def quarter_x(rel, q):
        return pl.ds(pl.multiple_of(rel * 256 + core * 128 + q * 16, 16), 16)

    def quarter_z(rel, q):
        return pl.ds(pl.multiple_of(rel * 256 + core * 128 + 64 + q * 16, 16), 16)

    def core_rows(rel, which):
        return pl.ds(pl.multiple_of(rel * 256 + which * 128, 128), 128)

    def step0(rel):
        pair_bands(rel, NC - 1)
        flight[rel] = [send(m.at[:, core_rows(rel, oc), :], r0.at[rel], G, rel * 26, other)]

    def landed(rel):
        for copy in flight[rel]:
            copy.wait_recv()
        flight[rel] = []

    def step1(rel):
        landed(rel)
        rows = core_rows(rel, core)
        m[:, rows, :] = m[:, rows, :] + r0[rel]
        for k in (1, 2, 3):
            to_x, to_z = (x + k) % 4, (z + k) % 4
            flight[rel] += [
                send(m.at[:, quarter_x(rel, to_x), :], r1.at[rel, 0, k - 1], G, rel * 26 + k, along_x[k - 1]),
                send(m.at[:, quarter_z(rel, to_z), :], r1.at[rel, 1, k - 1], G, rel * 26 + 3 + k, along_z[k - 1]),
            ]

    def step2(rel):
        landed(rel)
        for part, rows in ((0, quarter_x(rel, x)), (1, quarter_z(rel, z))):
            s[rel, part] = (m[:, rows, :] + r1[rel, part, 0]) + (r1[rel, part, 1] + r1[rel, part, 2])
        for k in (1, 2, 3):
            to_x, to_z = (x + k) % 4, (z + k) % 4
            flight[rel] += [
                send(s.at[rel, 0, to_z // 2, :, lanes_of(to_z)], r2.at[rel, 0, k - 1], G, rel * 26 + 6 + k, along_z[k - 1]),
                send(s.at[rel, 1, to_x // 2, :, lanes_of(to_x)], r2.at[rel, 1, k - 1], G, rel * 26 + 9 + k, along_x[k - 1]),
            ]

    def step3(rel):
        landed(rel)
        done = []
        for part, q, rows in ((0, z, quarter_x(rel, x)), (1, x, quarter_z(rel, z))):
            total = s[rel, part, q // 2, :, lanes_of(q)] + r2[rel, part, 0]
            total = total + (r2[rel, part, 1] + r2[rel, part, 2])
            w[q // 2, rows, lanes_of(q)] = total * wv[q // 2, :, lanes_of(q)]
            done.append(w.at[q // 2, rows, lanes_of(q)])
        for k in (1, 2, 3):
            flight[rel] += [
                send(done[0], done[0], G, rel * 26 + 12 + k, along_z[k - 1]),
                send(done[1], done[1], G, rel * 26 + 15 + k, along_x[k - 1]),
            ]

    def step4(rel):
        landed(rel)
        for_x, for_z = w.at[:, quarter_x(rel, x), :], w.at[:, quarter_z(rel, z), :]
        for k in (1, 2, 3):
            flight[rel] += [
                send(for_x, for_x, G, rel * 26 + 18 + k, along_x[k - 1]),
                send(for_z, for_z, G, rel * 26 + 21 + k, along_z[k - 1]),
            ]

    def step5(rel):
        landed(rel)
        block = w.at[:, core_rows(rel, core), :]
        flight[rel] = [send(block, block, G, rel * 26 + 25, other)]

    def step6(rel):
        landed(rel)
        left = []
        for half in (0, 1):
            plain = split(w[half, rel * 256 : rel * 256 + 256, :])
            turned = [
                jnp.concatenate([-v[64:128], v[:64], -v[192:], v[128:192]], axis=0) for v in plain
            ]
            left.append((plain, turned))

        def body(part, _):
            total = None
            for half in (0, 1):
                for imag in (0, 1):
                    rows = pl.ds(pl.multiple_of(imag * HALF + part * 512, 512), 512)
                    term = three(nt, left[half][imag], (p_hi[half, rows, :], p_lo[half, rows, :]))
                    total = term if total is None else total + term
            c[rel, 0, part] = total[:COLS]
            c[rel, 1, part] = total[COLS:]
            return 0

        lax.fori_loop(0, 2, body, 0)

    C = (c_s, c_r)
    relay = {}
    final = {}

    def step7(rel):
        if rel == 0:
            for i, part in enumerate((p, o)):
                relay[0, i] = send(c.at[0, part, 0], rl.at[0, i], C, i, up)
                relay[1, i] = send(c.at[0, part, 1], rl.at[1, i], C, 2 + i, down)
        if rel == 2:
            for i, part in enumerate((p, o)):
                for way, source, to in ((0, 1, up), (1, 2, down)):
                    free, held = 1 - way, way
                    final[way, i, free] = send(
                        c.at[source, part, free], fin.at[way, i, free], C, 4 + way * 4 + i * 2 + free, to
                    )
                for way, source, to in ((0, 1, up), (1, 2, down)):
                    held = way
                    relay[way, i].wait_recv()
                    c[source, part, held] = c[source, part, held] + rl[way, i]
                    final[way, i, held] = send(
                        c.at[source, part, held], fin.at[way, i, held], C, 4 + way * 4 + i * 2 + held, to
                    )

    steps = (step0, step1, step2, step3, step4, step5, step6, step7)
    for t in range(len(steps) + 3):
        for rel in range(4):
            if 0 <= t - rel < len(steps):
                steps[t - rel](rel)

    across = []
    for l in (0, 1):
        final[0, 0, l].wait_recv()
        final[1, 0, l].wait_recv()
        c[3, p, l] = c[3, p, l] + (fin[0, 0, l] + fin[1, 0, l])
        across.append(send(c.at[3, p, l], zin.at[l], C, 12 + l, pair))
    for l in (0, 1):
        final[0, 1, l].wait_recv()
        final[1, 1, l].wait_recv()
        lanes = pl.ds(pl.multiple_of(o * HALF + l * 512, 512), 512)
        out[:, lanes] = at[:, lanes] - (c[3, o, l] + (fin[0, 1, l] + fin[1, 1, l]))
    for l in (0, 1):
        across[l].wait_recv()
        lanes = pl.ds(pl.multiple_of(p * HALF + l * 512, 512), 512)
        out[:, lanes] = at[:, lanes] - zin[l]

    for copy in sent:
        copy.wait_send()


def projected(at, psi, wt):
    dma = pltpu.SemaphoreType.DMA
    vmem = pl.BlockSpec(memory_space=pltpu.VMEM)
    return pl.pallas_call(
        kernel,
        out_shape=jax.ShapeDtypeStruct((COLS, SLAB), F32),
        in_specs=[vmem, pl.BlockSpec(memory_space=pl.ANY), vmem],
        out_specs=vmem,
        scratch_shapes=[
            pltpu.VMEM((2, HALF, BANDS), F32),
            pltpu.VMEM((2, HALF, BANDS), F32),
            pltpu.VMEM((4, 2, COLS, HALF), F32),
            pltpu.VMEM((1024, 2 * HALF), BF16),
            pltpu.VMEM((1024, 2 * HALF), BF16),
            pltpu.VMEM((2, 2 * HALF, BANDS), BF16),
            pltpu.VMEM((2, 2 * HALF, BANDS), BF16),
            pltpu.VMEM((2, 16, BANDS), F32),
            pltpu.VMEM((2, 1024, BANDS), F32),
            pltpu.VMEM((2, 1024, BANDS), F32),
            pltpu.VMEM((4, 2, 2, COLS, 512), F32),
            pltpu.VMEM((4, 2, 128, BANDS), F32),
            pltpu.VMEM((4, 2, 3, 2, 16, BANDS), F32),
            pltpu.VMEM((4, 2, 3, 16, 128), F32),
            pltpu.VMEM((4, 2, 2, 16, BANDS), F32),
            pltpu.VMEM((2, 2, COLS, 512), F32),
            pltpu.VMEM((2, 2, 2, COLS, 512), F32),
            pltpu.VMEM((2, COLS, 512), F32),
            dma, dma((8,)), dma((8,)), dma((NC,)), dma((NC,)),
            dma((104,)), dma((104,)), dma((14,)), dma((14,)),
        ],
        compiler_params=pltpu.CompilerParams(
            collective_id=0, has_side_effects=True, vmem_limit_bytes=52 * 1024 * 1024
        ),
    )(at, psi, wt)


def per_device(psi, dpsi, band_weight, panel_band, slab_offset):
    offset = slab_offset[lax.axis_index("ga")]
    aligned = jnp.roll(jnp.swapaxes(dpsi, 1, 2), -offset, axis=2).reshape(COLS, SLAB)
    table = band_weight.reshape(-1, PANEL)
    chosen = panel_band[:, None] == jnp.arange(table.shape[0], dtype=jnp.int32)[None, :]
    weight = jnp.sum(jnp.where(chosen[:, :, None], table[None], 0.0), axis=1).reshape(1, BANDS)
    result = projected(aligned, psi, jnp.broadcast_to(weight, (16, BANDS)))
    return jnp.swapaxes(jnp.roll(result.reshape(2, COLS // 2, SLAB), offset, axis=2), 1, 2)


def solution(mesh):
    in_specs = (P(None, "ga", "ba"), P(None, "ga", "ba"), P(), P("ba"), P())
    out_specs = P(None, "ga", "ba")
    return jax.shard_map(
        per_device, mesh=mesh, in_specs=in_specs, out_specs=out_specs, check_vma=False
    )
```

```python
import jax
import jax.numpy as jnp
from jax import lax
from jax.experimental import pallas as pl
from jax.experimental.pallas import tpu as pltpu
from jax.sharding import PartitionSpec as P

F32, BF16 = jnp.float32, jnp.bfloat16
PANEL = 128
SLAB = 2048
BANDS = 256
COLS = 128
HALF = 768
BOTH = SLAB - 2 * HALF
MINE = HALF + BOTH
PIECES = (0, 64, 256, 512, 640, HALF)
LAST = PIECES[-2]
L2, L1 = HALF // 2, BOTH // 2
NT = (((1,), (1,)), ((), ()))


def split(value):
    high = value.astype(BF16)
    return high, (value - high.astype(F32)).astype(BF16)


def three(dot, left, right):
    return dot(left[0], right[0]) + (dot(left[0], right[1]) + dot(left[1], right[0]))


def nn(left, right):
    return jnp.dot(left, right, preferred_element_type=F32)


def nt(left, right):
    return lax.dot_general(left, right, NT, preferred_element_type=F32)


def kernel(
    raw_hbm, psi, table, panels, offsets, out,
    raw, at, psi_o, psi_p, a_v, a_hi, a_lo, o_hi, o_lo, p_hi, p_lo, ws, wv, m, w, c2, c1,
    r0, r1, r2, s, rl2, rl1, fin2, fin1, zin, zg,
    local_sem, a_s, a_r, p_s, p_r, g_s, g_r, c_s, c_r,
):
    ga, ba = lax.axis_index("ga"), lax.axis_index("ba")
    x, zhi, core = ga // 4, (ga // 2) % 2, ga % 2
    y, o = ba // 2, ba % 2
    p = 1 - o
    z = zhi * 2 + o
    oc = 1 - core

    def device(x=x, z=z, y=y, core=core):
        return (x * 4 + (z // 2) * 2 + core, y * 2 + z % 2)

    pair = device(z=zhi * 2 + p)
    up, down = device(y=(y + 1) % 4), device(y=(y + 3) % 4)
    other = device(core=oc)
    along_x = [device(x=(x + k) % 4) for k in (1, 2, 3)]
    along_z = [device(z=(z + k) % 4) for k in (1, 2, 3)]

    sent = []

    def send(src, dst, sems, index, to):
        copy = pltpu.make_async_remote_copy(
            src_ref=src, dst_ref=dst, send_sem=sems[0].at[index], recv_sem=sems[1].at[index],
            device_id=to, device_id_type=pl.DeviceIdType.MESH,
        )
        copy.start()
        sent.append(copy)
        return copy

    def half_at(which):
        return pl.multiple_of(which * HALF, HALF)

    barrier = pltpu.get_barrier_semaphore()
    peers = [up, down, other, *along_x, *along_z]
    for peer in peers:
        pl.semaphore_signal(barrier, inc=1, device_id=peer, device_id_type=pl.DeviceIdType.MESH)

    local = [
        pltpu.make_async_copy(raw_hbm, raw, local_sem.at[0]),
        pltpu.make_async_copy(
            psi.at[:, pl.ds(half_at(o), HALF), :], psi_o.at[:, pl.ds(0, HALF), :], local_sem.at[1]
        ),
        pltpu.make_async_copy(
            psi.at[:, pl.ds(2 * HALF, BOTH), :], psi_o.at[:, pl.ds(HALF, BOTH), :], local_sem.at[2]
        ),
    ]
    for copy in local:
        copy.start()

    waves = []

    def send_waves(k):
        first, count = PIECES[k], PIECES[k + 1] - PIECES[k]
        waves.append(
            send(
                psi.at[:, pl.ds(pl.multiple_of(p * HALF + first, 64), count), :],
                psi_p.at[:, pl.ds(first, count), :], (p_s, p_r), k, pair,
            )
        )

    local[0].wait()

    offset = offsets[ga]
    lane = lax.broadcasted_iota(jnp.int32, (16, 128), 1)

    def align(k, _):
        rows = pl.ds(pl.multiple_of(k * 16, 16), 16)
        tiles = [raw[rows, t * 128 : (t + 1) * 128] for t in range(16)]
        for bit in (10, 9, 8, 7, 6, 5, 4, 3, 2, 1, 0):
            turn = jnp.full((16, 128), (offset >> bit) & 1, jnp.int32) != 0
            if bit >= 7:
                moved = [tiles[(t + (1 << (bit - 7))) % 16] for t in range(16)]
            else:
                rolled = [pltpu.roll(tile, 128 - (1 << bit), 1) for tile in tiles]
                inside = lane < 128 - (1 << bit)
                moved = [jnp.where(inside, rolled[t], rolled[(t + 1) % 16]) for t in range(16)]
            tiles = [jnp.where(turn, new, old) for new, old in zip(moved, tiles)]
        for t, value in enumerate(tiles):
            if t * 128 < 2 * HALF:
                half, first = divmod(t * 128, HALF)
                at[half, rows, first : first + 128] = value
            else:
                first = t * 128 - HALF
                at[0, rows, first : first + 128] = value
                at[1, rows, first : first + 128] = value
        return 0

    lax.fori_loop(0, COLS // 16, align, 0)

    row = lax.broadcasted_iota(jnp.int32, (16, PANEL), 0)
    for k in (0, 1):
        chosen = jnp.where(row == jnp.full((16, PANEL), panels[k], jnp.int32), table[...], 0.0)
        ws[:, k * PANEL : (k + 1) * PANEL] = jnp.broadcast_to(
            jnp.sum(chosen, axis=0, keepdims=True), (16, PANEL)
        )
    wv[o] = ws[...]

    pl.semaphore_wait(barrier, len(peers))
    send_waves(0)

    A = (a_s, a_r)
    a_pair = send(at.at[p], a_v.at[3, o], A, 0, pair)
    a_up_o = send(at.at[o], a_v.at[2, o], A, 1, up)
    a_down_o = send(at.at[o], a_v.at[1, o], A, 2, down)
    w_pair = send(ws, wv.at[o], A, 7, pair)
    for k in range(1, len(PIECES) - 1):
        send_waves(k)

    def keep_columns(value, rel, half):
        rows = rel * 256 + half * COLS
        top = pl.ds(pl.multiple_of(rows, 64), 64)
        bottom = pl.ds(pl.multiple_of(rows + 64, 64), 64)
        for ref, part in zip((a_hi, a_lo), split(value)):
            ref[top, :MINE] = part[:64]
            ref[bottom, :MINE] = part[64:]
            ref[top, MINE:] = part[64:]
            ref[bottom, MINE:] = -part[:64]

    def keep_waves(ref, high_ref, low_ref, length, first, count):
        for part in (0, 1):
            high, low = split(ref[part, first : first + count, :])
            high_ref[part * length + first : part * length + first + count, :] = high
            low_ref[part * length + first : part * length + first + count, :] = low

    def keep_piece(k):
        waves[k].wait_recv()
        keep_waves(psi_p, p_hi, p_lo, HALF, PIECES[k], PIECES[k + 1] - PIECES[k])

    keep_columns(at[o], 3, o)
    local[1].wait()
    local[2].wait()
    keep_waves(psi_o, o_hi, o_lo, MINE, 0, MINE)
    keep_piece(0)

    a_pair.wait_recv()
    a_up_p = send(a_v.at[3, p], a_v.at[2, p], A, 3, up)
    a_down_p = send(a_v.at[3, p], a_v.at[1, p], A, 4, down)
    a_up_o.wait_recv()
    far_o = send(a_v.at[2, o], a_v.at[0, o], A, 5, up)
    keep_columns(a_v[3, p], 3, p)
    keep_columns(a_v[2, o], 2, o)
    a_down_o.wait_recv()
    keep_columns(a_v[1, o], 1, o)
    keep_piece(1)
    a_down_p.wait_recv()
    far_p = send(a_v.at[1, p], a_v.at[0, p], A, 6, down)
    keep_columns(a_v[1, p], 1, p)
    a_up_p.wait_recv()
    keep_columns(a_v[2, p], 2, p)
    keep_piece(2)
    w_pair.wait_recv()

    def own_bands(rel):
        rows = pl.ds(pl.multiple_of(rel * 256, 256), 256)
        m[o, rows, :] = three(nn, (a_hi[rows, :], a_lo[rows, :]), (o_hi[...], o_lo[...]))

    def pair_bands(rel, first, last):
        rows = pl.ds(pl.multiple_of(rel * 256, 256), 256)
        total = None
        for part in (0, 1):
            ks, rs = pl.ds(part * MINE + first, last - first), pl.ds(part * HALF + first, last - first)
            term = three(nn, (a_hi[rows, ks], a_lo[rows, ks]), (p_hi[rs, :], p_lo[rs, :]))
            total = term if total is None else total + term
        return rows, total

    def early(rel, _):
        own_bands(rel)
        rows, total = pair_bands(rel, 0, PIECES[3])
        m[p, rows, :] = total
        return 0

    lax.fori_loop(1, 4, early, 0)
    far_o.wait_recv()
    keep_columns(a_v[0, o], 0, o)
    far_p.wait_recv()
    keep_columns(a_v[0, p], 0, p)
    lax.fori_loop(0, 1, early, 0)
    keep_piece(3)

    def later(rel, _):
        rows, total = pair_bands(rel, PIECES[3], LAST)
        m[p, rows, :] = m[p, rows, :] + total
        return 0

    lax.fori_loop(0, 4, later, 0)
    keep_piece(4)

    G = (g_s, g_r)
    flight = {}

    def rows_of(rel, who, length, first=0):
        return pl.ds(pl.multiple_of(rel * 256 + first + who * length, 16), length)

    def lanes_of(q):
        return pl.ds(pl.multiple_of((q % 2) * 128, 128), 128)

    def quarter_x(rel, q):
        return pl.ds(pl.multiple_of(rel * 256 + core * 128 + q * 16, 16), 16)

    def quarter_z(rel, q):
        return pl.ds(pl.multiple_of(rel * 256 + core * 128 + 64 + q * 16, 16), 16)

    def core_rows(rel, which):
        return pl.ds(pl.multiple_of(rel * 256 + which * 128, 128), 128)

    def step0(rel):
        rows, total = pair_bands(rel, LAST, HALF)
        m[p, rows, :] = m[p, rows, :] + total
        flight[rel] = [send(m.at[:, core_rows(rel, oc), :], r0.at[rel], G, rel * 26, other)]

    def landed(rel):
        for copy in flight[rel]:
            copy.wait_recv()
        flight[rel] = []

    def step1(rel):
        landed(rel)
        rows = core_rows(rel, core)
        m[:, rows, :] = m[:, rows, :] + r0[rel]
        for k in (1, 2, 3):
            to_x, to_z = (x + k) % 4, (z + k) % 4
            flight[rel] += [
                send(m.at[:, quarter_x(rel, to_x), :], r1.at[rel, 0, k - 1], G, rel * 26 + k, along_x[k - 1]),
                send(m.at[:, quarter_z(rel, to_z), :], r1.at[rel, 1, k - 1], G, rel * 26 + 3 + k, along_z[k - 1]),
            ]

    def step2(rel):
        landed(rel)
        for part, rows in ((0, quarter_x(rel, x)), (1, quarter_z(rel, z))):
            s[rel, part] = (m[:, rows, :] + r1[rel, part, 0]) + (r1[rel, part, 1] + r1[rel, part, 2])
        for k in (1, 2, 3):
            to_x, to_z = (x + k) % 4, (z + k) % 4
            flight[rel] += [
                send(s.at[rel, 0, to_z // 2, :, lanes_of(to_z)], r2.at[rel, 0, k - 1], G, rel * 26 + 6 + k, along_z[k - 1]),
                send(s.at[rel, 1, to_x // 2, :, lanes_of(to_x)], r2.at[rel, 1, k - 1], G, rel * 26 + 9 + k, along_x[k - 1]),
            ]

    def step3(rel):
        landed(rel)
        done = []
        for part, q, rows in ((0, z, quarter_x(rel, x)), (1, x, quarter_z(rel, z))):
            total = s[rel, part, q // 2, :, lanes_of(q)] + r2[rel, part, 0]
            total = total + (r2[rel, part, 1] + r2[rel, part, 2])
            w[q // 2, rows, lanes_of(q)] = total * wv[q // 2, :, lanes_of(q)]
            done.append(w.at[q // 2, rows, lanes_of(q)])
        for k in (1, 2, 3):
            flight[rel] += [
                send(done[0], done[0], G, rel * 26 + 12 + k, along_z[k - 1]),
                send(done[1], done[1], G, rel * 26 + 15 + k, along_x[k - 1]),
            ]

    def step4(rel):
        landed(rel)
        for_x, for_z = w.at[:, quarter_x(rel, x), :], w.at[:, quarter_z(rel, z), :]
        for k in (1, 2, 3):
            flight[rel] += [
                send(for_x, for_x, G, rel * 26 + 18 + k, along_x[k - 1]),
                send(for_z, for_z, G, rel * 26 + 21 + k, along_z[k - 1]),
            ]

    def step5(rel):
        landed(rel)
        block = w.at[:, core_rows(rel, core), :]
        flight[rel] = [send(block, block, G, rel * 26 + 25, other)]

    C = (c_s, c_r)
    pairs = {}

    def step6(rel):
        landed(rel)
        left = []
        for half in (o, p):
            plain = split(w[half, rel * 256 : rel * 256 + 256, :])
            left.append((plain, [
                jnp.concatenate([-v[64:128], v[:64], -v[192:], v[128:192]], axis=0) for v in plain
            ]))
        mine, theirs = left

        def both(l, _):
            total = None
            for imag in (0, 1):
                rows = pl.ds(pl.multiple_of(imag * MINE + HALF + l * L1, L1), L1)
                term = three(nt, mine[imag], (o_hi[rows, :], o_lo[rows, :]))
                total = term if total is None else total + term
            c1[rel, 0, l] = total[:COLS]
            c1[rel, 1, l] = total[COLS:]
            return 0

        lax.fori_loop(0, 2, both, 0)
        pairs[rel] = send(c1.at[rel, p], zg.at[rel], C, 20 + rel, pair)

        def alone(l, _):
            total = None
            for imag in (0, 1):
                rows = pl.ds(pl.multiple_of(imag * MINE + l * L2, 128), L2)
                term = three(nt, mine[imag], (o_hi[rows, :], o_lo[rows, :]))
                total = term if total is None else total + term
                rows = pl.ds(pl.multiple_of(imag * HALF + l * L2, L2), L2)
                total = total + three(nt, theirs[imag], (p_hi[rows, :], p_lo[rows, :]))
            c2[rel, 0, l] = total[:COLS]
            c2[rel, 1, l] = total[COLS:]
            return 0

        lax.fori_loop(0, 2, alone, 0)

    ways = ((0, 1, up), (1, 2, down))
    relay, final = {}, {}

    def piece(rel, i, l):
        return (c2.at[rel, p, l], c2.at[rel, o, l], c1.at[rel, o, l])[i]

    def summed_over_pair(rel):
        pairs[rel].wait_recv()
        c1[rel, o] = c1[rel, o] + zg[rel]

    def relay_slot(way, i):
        return rl1.at[way] if i == 2 else rl2.at[way, i]

    def final_slot(way, i, l):
        return fin1.at[way, l] if i == 2 else fin2.at[way, i, l]

    def send_final(way, i, l):
        _, rel, to = ways[way]
        final[way, i, l] = send(
            piece(rel, i, l), final_slot(way, i, l), C, 6 + way * 6 + i * 2 + l, to
        )

    def step7(rel):
        if rel == 0:
            for i in (0, 1, 2):
                if i == 2:
                    summed_over_pair(0)
                for way, _, to in ways:
                    relay[way, i] = send(piece(0, i, way), relay_slot(way, i), C, way * 3 + i, to)
        if rel == 1:
            send_final(0, 0, 1)
        if rel == 2:
            send_final(1, 0, 0)
            for i in (0, 1, 2):
                for way, source, _ in ways:
                    if i == 2:
                        summed_over_pair(source)
                    if i > 0:
                        send_final(way, i, 1 - way)
                for way, source, _ in ways:
                    relay[way, i].wait_recv()
                    held = piece(source, i, way)
                    held[...] = held[...] + relay_slot(way, i)[...]
                    send_final(way, i, way)

    steps = (step0, step1, step2, step3, step4, step5, step6, step7)
    for t in range(len(steps) + 3):
        for rel in range(4):
            if 0 <= t - rel < len(steps):
                steps[t - rel](rel)

    def arrived(i, l):
        final[0, i, l].wait_recv()
        final[1, i, l].wait_recv()
        return piece(3, i, l)[...] + (final_slot(0, i, l)[...] + final_slot(1, i, l)[...])

    across = []
    for l in (0, 1):
        c2[3, p, l] = arrived(0, l)
        across.append(send(c2.at[3, p, l], zin.at[l], C, 18 + l, pair))
    for l in (0, 1):
        lanes = pl.ds(pl.multiple_of(o * HALF + l * L2, 128), L2)
        out[:, lanes] = at[o, :, l * L2 : (l + 1) * L2] - arrived(1, l)
    summed_over_pair(3)
    for l in (0, 1):
        first = HALF + l * L1
        out[:, HALF + first : HALF + first + L1] = at[o, :, first : first + L1] - arrived(2, l)
    for l in (0, 1):
        across[l].wait_recv()
        lanes = pl.ds(pl.multiple_of(p * HALF + l * L2, 128), L2)
        out[:, lanes] = at[p, :, l * L2 : (l + 1) * L2] - zin[l]

    for copy in sent:
        copy.wait_send()


def projected(raw, psi, table, panels, offsets):
    dma = pltpu.SemaphoreType.DMA
    vmem, smem = pl.BlockSpec(memory_space=pltpu.VMEM), pl.BlockSpec(memory_space=pltpu.SMEM)
    anywhere = pl.BlockSpec(memory_space=pl.ANY)
    return pl.pallas_call(
        kernel,
        out_shape=jax.ShapeDtypeStruct((COLS, SLAB), F32),
        in_specs=[anywhere, anywhere, vmem, smem, smem],
        out_specs=vmem,
        scratch_shapes=[
            pltpu.VMEM((COLS, SLAB), F32),
            pltpu.VMEM((2, COLS, MINE), F32),
            pltpu.VMEM((2, MINE, BANDS), F32),
            pltpu.VMEM((2, HALF, BANDS), F32),
            pltpu.VMEM((4, 2, COLS, MINE), F32),
            pltpu.VMEM((1024, 2 * MINE), BF16),
            pltpu.VMEM((1024, 2 * MINE), BF16),
            pltpu.VMEM((2 * MINE, BANDS), BF16),
            pltpu.VMEM((2 * MINE, BANDS), BF16),
            pltpu.VMEM((2 * HALF, BANDS), BF16),
            pltpu.VMEM((2 * HALF, BANDS), BF16),
            pltpu.VMEM((16, BANDS), F32),
            pltpu.VMEM((2, 16, BANDS), F32),
            pltpu.VMEM((2, 1024, BANDS), F32),
            pltpu.VMEM((2, 1024, BANDS), F32),
            pltpu.VMEM((4, 2, 2, COLS, L2), F32),
            pltpu.VMEM((4, 2, 2, COLS, L1), F32),
            pltpu.VMEM((4, 2, 128, BANDS), F32),
            pltpu.VMEM((4, 2, 3, 2, 16, BANDS), F32),
            pltpu.VMEM((4, 2, 3, 16, 128), F32),
            pltpu.VMEM((4, 2, 2, 16, BANDS), F32),
            pltpu.VMEM((2, 2, COLS, L2), F32),
            pltpu.VMEM((2, COLS, L1), F32),
            pltpu.VMEM((2, 2, 2, COLS, L2), F32),
            pltpu.VMEM((2, 2, COLS, L1), F32),
            pltpu.VMEM((2, COLS, L2), F32),
            pltpu.VMEM((4, 2, COLS, L1), F32),
            dma((3,)), dma((8,)), dma((8,)), dma((5,)), dma((5,)),
            dma((104,)), dma((104,)), dma((24,)), dma((24,)),
        ],
        compiler_params=pltpu.CompilerParams(
            collective_id=0, has_side_effects=True, vmem_limit_bytes=56 * 1024 * 1024
        ),
    )(raw, psi, table, panels, offsets)


def per_device(psi, dpsi, band_weight, panel_band, slab_offset):
    raw = jnp.swapaxes(dpsi, 1, 2).reshape(COLS, SLAB)
    result = projected(raw, psi, band_weight.reshape(-1, PANEL), panel_band, slab_offset)
    offset = slab_offset[lax.axis_index("ga")]
    return jnp.swapaxes(jnp.roll(result.reshape(2, COLS // 2, SLAB), offset, axis=2), 1, 2)


def solution(mesh):
    in_specs = (P(None, "ga", "ba"), P(None, "ga", "ba"), P(), P("ba"), P())
    out_specs = P(None, "ga", "ba")
    return jax.shard_map(
        per_device, mesh=mesh, in_specs=in_specs, out_specs=out_specs, check_vma=False
    )
```

```python
import jax
import jax.numpy as jnp
from jax import lax
from jax.experimental import pallas as pl
from jax.experimental.pallas import tpu as pltpu
from jax.sharding import PartitionSpec as P

F32, BF16 = jnp.float32, jnp.bfloat16
PANEL = 128
SLAB = 2048
BANDS = 256
COLS = 128
HALF = 768
BOTH = SLAB - 2 * HALF
MINE = HALF + BOTH
PIECES = (0, 64, 256, 512, 640, HALF)
LAST = PIECES[-2]
L2, L1 = HALF // 2, BOTH // 2
NT = (((1,), (1,)), ((), ()))


def split(value):
    high = value.astype(BF16)
    return high, (value - high.astype(F32)).astype(BF16)


def three(dot, left, right):
    return dot(left[0], right[0]) + (dot(left[0], right[1]) + dot(left[1], right[0]))


def nn(left, right):
    return jnp.dot(left, right, preferred_element_type=F32)


def nt(left, right):
    return lax.dot_general(left, right, NT, preferred_element_type=F32)


def kernel(
    raw_hbm, psi, table_hbm, panels_hbm, offsets_hbm, out,
    raw, table, panels, offsets, at, psi_o, psi_p, a_v, a_hi, a_lo, o_hi, o_lo, p_hi, p_lo, ws, wv, m, w, c2, c1,
    r0, r1, r2, s, rl2, rl1, fin2, fin1, zin, zg,
    local_sem, a_s, a_r, p_s, p_r, g_s, g_r, c_s, c_r,
):
    ga, ba = lax.axis_index("ga"), lax.axis_index("ba")
    x, zhi, core = ga // 4, (ga // 2) % 2, ga % 2
    y, o = ba // 2, ba % 2
    p = 1 - o
    z = zhi * 2 + o
    oc = 1 - core

    def device(x=x, z=z, y=y, core=core):
        return (x * 4 + (z // 2) * 2 + core, y * 2 + z % 2)

    pair = device(z=zhi * 2 + p)
    up, down = device(y=(y + 1) % 4), device(y=(y + 3) % 4)
    other = device(core=oc)
    along_x = [device(x=(x + k) % 4) for k in (1, 2, 3)]
    along_z = [device(z=(z + k) % 4) for k in (1, 2, 3)]

    sent = []

    def send(src, dst, sems, index, to):
        copy = pltpu.make_async_remote_copy(
            src_ref=src, dst_ref=dst, send_sem=sems[0].at[index], recv_sem=sems[1].at[index],
            device_id=to, device_id_type=pl.DeviceIdType.MESH,
        )
        copy.start()
        sent.append(copy)
        return copy

    def half_at(which):
        return pl.multiple_of(which * HALF, HALF)

    barrier = pltpu.get_barrier_semaphore()
    peers = [up, down, other, *along_x, *along_z]
    for peer in peers:
        pl.semaphore_signal(barrier, inc=1, device_id=peer, device_id_type=pl.DeviceIdType.MESH)

    small = [
        pltpu.make_async_copy(offsets_hbm, offsets, local_sem.at[3]),
        pltpu.make_async_copy(table_hbm, table, local_sem.at[4]),
        pltpu.make_async_copy(panels_hbm, panels, local_sem.at[5]),
    ]
    local = [
        pltpu.make_async_copy(raw_hbm, raw, local_sem.at[0]),
        pltpu.make_async_copy(
            psi.at[:, pl.ds(half_at(o), HALF), :], psi_o.at[:, pl.ds(0, HALF), :], local_sem.at[1]
        ),
        pltpu.make_async_copy(
            psi.at[:, pl.ds(2 * HALF, BOTH), :], psi_o.at[:, pl.ds(HALF, BOTH), :], local_sem.at[2]
        ),
    ]
    for copy in small + local:
        copy.start()

    waves = []

    def send_waves(k):
        first, count = PIECES[k], PIECES[k + 1] - PIECES[k]
        waves.append(
            send(
                psi.at[:, pl.ds(pl.multiple_of(p * HALF + first, 64), count), :],
                psi_p.at[:, pl.ds(first, count), :], (p_s, p_r), k, pair,
            )
        )

    pl.semaphore_wait(barrier, len(peers))
    send_waves(0)
    for copy in small:
        copy.wait()
    local[0].wait()

    offset = offsets[ga]
    lane = lax.broadcasted_iota(jnp.int32, (16, 128), 1)

    def align(k, _):
        rows = pl.ds(pl.multiple_of(k * 16, 16), 16)
        tiles = [raw[rows, t * 128 : (t + 1) * 128] for t in range(16)]
        for bit in (10, 9, 8, 7, 6, 5, 4, 3, 2, 1, 0):
            turn = jnp.full((16, 128), (offset >> bit) & 1, jnp.int32) != 0
            if bit >= 7:
                moved = [tiles[(t + (1 << (bit - 7))) % 16] for t in range(16)]
            else:
                rolled = [pltpu.roll(tile, 128 - (1 << bit), 1) for tile in tiles]
                inside = lane < 128 - (1 << bit)
                moved = [jnp.where(inside, rolled[t], rolled[(t + 1) % 16]) for t in range(16)]
            tiles = [jnp.where(turn, new, old) for new, old in zip(moved, tiles)]
        for t, value in enumerate(tiles):
            if t * 128 < 2 * HALF:
                half, first = divmod(t * 128, HALF)
                at[half, rows, first : first + 128] = value
            else:
                first = t * 128 - HALF
                at[0, rows, first : first + 128] = value
                at[1, rows, first : first + 128] = value
        return 0

    lax.fori_loop(0, COLS // 16, align, 0)

    row = lax.broadcasted_iota(jnp.int32, (16, PANEL), 0)
    for k in (0, 1):
        chosen = jnp.where(row == jnp.full((16, PANEL), panels[k], jnp.int32), table[...], 0.0)
        ws[:, k * PANEL : (k + 1) * PANEL] = jnp.broadcast_to(
            jnp.sum(chosen, axis=0, keepdims=True), (16, PANEL)
        )
    wv[o] = ws[...]

    A = (a_s, a_r)
    a_pair = send(at.at[p], a_v.at[3, o], A, 0, pair)
    a_up_o = send(at.at[o], a_v.at[2, o], A, 1, up)
    a_down_o = send(at.at[o], a_v.at[1, o], A, 2, down)
    w_pair = send(ws, wv.at[o], A, 7, pair)
    for k in range(1, len(PIECES) - 1):
        send_waves(k)

    def keep_columns(value, rel, half):
        rows = rel * 256 + half * COLS
        top = pl.ds(pl.multiple_of(rows, 64), 64)
        bottom = pl.ds(pl.multiple_of(rows + 64, 64), 64)
        for ref, part in zip((a_hi, a_lo), split(value)):
            ref[top, :MINE] = part[:64]
            ref[bottom, :MINE] = part[64:]
            ref[top, MINE:] = part[64:]
            ref[bottom, MINE:] = -part[:64]

    def keep_waves(ref, high_ref, low_ref, length, first, count):
        for part in (0, 1):
            high, low = split(ref[part, first : first + count, :])
            high_ref[part * length + first : part * length + first + count, :] = high
            low_ref[part * length + first : part * length + first + count, :] = low

    def keep_piece(k):
        waves[k].wait_recv()
        keep_waves(psi_p, p_hi, p_lo, HALF, PIECES[k], PIECES[k + 1] - PIECES[k])

    keep_columns(at[o], 3, o)
    local[1].wait()
    local[2].wait()
    keep_waves(psi_o, o_hi, o_lo, MINE, 0, MINE)
    keep_piece(0)

    a_pair.wait_recv()
    a_up_p = send(a_v.at[3, p], a_v.at[2, p], A, 3, up)
    a_down_p = send(a_v.at[3, p], a_v.at[1, p], A, 4, down)
    a_up_o.wait_recv()
    far_o = send(a_v.at[2, o], a_v.at[0, o], A, 5, up)
    keep_columns(a_v[3, p], 3, p)
    keep_columns(a_v[2, o], 2, o)
    a_down_o.wait_recv()
    keep_columns(a_v[1, o], 1, o)
    keep_piece(1)
    a_down_p.wait_recv()
    far_p = send(a_v.at[1, p], a_v.at[0, p], A, 6, down)
    keep_columns(a_v[1, p], 1, p)
    a_up_p.wait_recv()
    keep_columns(a_v[2, p], 2, p)
    keep_piece(2)
    w_pair.wait_recv()

    def own_bands(rel):
        rows = pl.ds(pl.multiple_of(rel * 256, 256), 256)
        m[o, rows, :] = three(nn, (a_hi[rows, :], a_lo[rows, :]), (o_hi[...], o_lo[...]))

    def block_rows(rel):
        return pl.ds(pl.multiple_of(rel * 256, 256), 256)

    def pair_bands(rows, first, last):
        total = None
        for part in (0, 1):
            ks, rs = pl.ds(part * MINE + first, last - first), pl.ds(part * HALF + first, last - first)
            term = three(nn, (a_hi[rows, ks], a_lo[rows, ks]), (p_hi[rs, :], p_lo[rs, :]))
            total = term if total is None else total + term
        return rows, total

    def early(rel, _):
        own_bands(rel)
        rows, total = pair_bands(block_rows(rel), 0, PIECES[3])
        m[p, rows, :] = total
        return 0

    lax.fori_loop(1, 4, early, 0)
    far_o.wait_recv()
    keep_columns(a_v[0, o], 0, o)
    far_p.wait_recv()
    keep_columns(a_v[0, p], 0, p)
    lax.fori_loop(0, 1, early, 0)
    keep_piece(3)

    def later(rel, _):
        rows, total = pair_bands(block_rows(rel), PIECES[3], LAST)
        m[p, rows, :] = m[p, rows, :] + total
        return 0

    lax.fori_loop(0, 4, later, 0)
    keep_piece(4)

    G = (g_s, g_r)
    chunks = ((0, 128), (128, 128), (256, 256), (512, 256), (768, 256))
    flight = {}

    def quarter(n, part, q):
        first, length = chunks[n]
        return pl.ds(
            pl.multiple_of(first + (core * 2 + part) * (length // 4) + q * (length // 16), 8),
            length // 16,
        )

    def core_rows(n, which):
        first, length = chunks[n]
        return pl.ds(pl.multiple_of(first + which * (length // 2), 64), length // 2)

    def landed(n):
        for copy in flight[n]:
            copy.wait_recv()
        flight[n] = []

    def step0(n):
        first, length = chunks[n]
        rows, total = pair_bands(pl.ds(first, length), LAST, HALF)
        m[p, rows, :] = m[p, rows, :] + total
        to = r0.at[:, pl.ds(first // 2, length // 2), :]
        flight[n] = [send(m.at[:, core_rows(n, oc), :], to, G, n * 20, other)]

    def step1(n):
        landed(n)
        first, length = chunks[n]
        rows = core_rows(n, core)
        m[:, rows, :] = m[:, rows, :] + r0[:, first // 2 : (first + length) // 2, :]
        few = pl.ds(0, length // 16)
        for k in (1, 2, 3):
            to_x, to_z = (x + k) % 4, (z + k) % 4
            flight[n] += [
                send(m.at[:, quarter(n, 0, to_x), :], r1.at[n, 0, k - 1, :, few], G, n * 20 + k, along_x[k - 1]),
                send(m.at[:, quarter(n, 1, to_z), :], r1.at[n, 1, k - 1, :, few], G, n * 20 + 3 + k, along_z[k - 1]),
            ]

    def four(mine, ref, n, part):
        few = chunks[n][1] // 16
        return (mine + ref[n, part, 0, :, :few]) + (ref[n, part, 1, :, :few] + ref[n, part, 2, :, :few])

    def step2(n):
        landed(n)
        few = pl.ds(0, chunks[n][1] // 16)
        for part, q in ((0, x), (1, z)):
            s[n, part, :, few, :] = four(m[:, quarter(n, part, q), :], r1, n, part)
        for k in (1, 2, 3):
            flight[n] += [
                send(s.at[n, 0, :, few], r2.at[n, 0, k - 1, :, few], G, n * 20 + 6 + k, along_z[k - 1]),
                send(s.at[n, 1, :, few], r2.at[n, 1, k - 1, :, few], G, n * 20 + 9 + k, along_x[k - 1]),
            ]

    def step3(n):
        landed(n)
        few = chunks[n][1] // 16
        for part, q in ((0, x), (1, z)):
            w[:, quarter(n, part, q), :] = four(s[n, part, :, :few], r2, n, part) * wv[:, :few, :]
        for_x, for_z = w.at[:, quarter(n, 0, x), :], w.at[:, quarter(n, 1, z), :]
        for k in (1, 2, 3):
            flight[n] += [
                send(for_x, for_x, G, n * 20 + 12 + k, along_x[k - 1]),
                send(for_z, for_z, G, n * 20 + 15 + k, along_z[k - 1]),
            ]

    def step4(n):
        landed(n)
        block = w.at[:, core_rows(n, core), :]
        flight[n] = [send(block, block, G, n * 20 + 19, other)]

    C = (c_s, c_r)
    pairs = {}

    def corrections(n, after=None):
        landed(n)
        first, length = chunks[n]
        rel, blocks = first // 256, range(first % 256 // COLS, (first % 256 + length) // COLS)
        left = []
        for half in (o, p):
            plain = split(w[half, first : first + length, :])
            turned = []
            for v in plain:
                rows = [(-v[r + 64 : r + 128], v[r : r + 64]) for r in range(0, length, COLS)]
                turned.append(jnp.concatenate([part for two in rows for part in two], axis=0))
            left.append((plain, turned))
        mine, theirs = left

        def both(l):
            total = None
            for imag in (0, 1):
                rows = pl.ds(imag * MINE + HALF + l * L1, L1)
                term = three(nt, mine[imag], (o_hi[rows, :], o_lo[rows, :]))
                total = term if total is None else total + term
            for i, block in enumerate(blocks):
                c1[rel, block, l] = total[i * COLS : (i + 1) * COLS]

        def alone(l):
            total = None
            for imag in (0, 1):
                rows = pl.ds(imag * MINE + l * L2, L2)
                term = three(nt, mine[imag], (o_hi[rows, :], o_lo[rows, :]))
                total = term if total is None else total + term
                rows = pl.ds(imag * HALF + l * L2, L2)
                total = total + three(nt, theirs[imag], (p_hi[rows, :], p_lo[rows, :]))
            for i, block in enumerate(blocks):
                c2[rel, block, l] = total[i * COLS : (i + 1) * COLS]

        return both, alone

    ways = ((0, 1, up), (1, 2, down))
    relay, final = {}, {}

    def piece(rel, i, l):
        return (c2.at[rel, p, l], c2.at[rel, o, l], c1.at[rel, o, l])[i]

    def summed_over_pair(rel):
        pairs[rel].wait_recv()
        c1[rel, o] = c1[rel, o] + zg[rel]

    def final_slot(way, i, l):
        return fin1.at[way, l] if i == 2 else fin2.at[way, i, l]

    def send_final(way, i, l):
        _, rel, to = ways[way]
        final[way, i, l] = send(
            piece(rel, i, l), final_slot(way, i, l), C, 6 + way * 6 + i * 2 + l, to
        )

    def to_pair(rel):
        pairs[rel] = send(c1.at[rel, p], zg.at[rel], C, 20 + rel, pair)

    def step5(n):
        both, alone = corrections(n)
        if n < 2:
            for way, _, to in ways:
                alone(way)
                relay[way, n] = send(c2.at[0, n, way], rl2.at[way, n], C, way * 3 + n, to)
            both(0)
            both(1)
            if n == 1:
                to_pair(0)
        else:
            both(0)
            both(1)
            to_pair(n - 1)
            alone(1)
            alone(0)
        if n == 2:
            send_final(0, 0, 1)
            summed_over_pair(0)
            for way, _, to in ways:
                relay[way, 2] = send(piece(0, 2, way), rl1.at[way], C, way * 3 + 2, to)
        if n == 3:
            send_final(1, 0, 0)
            for way in (0, 1):
                relay[way, 0].wait_recv()
                relay[way, 1].wait_recv()
            for i in (0, 1, 2):
                for way, source, _ in ways:
                    if i == 2:
                        summed_over_pair(source)
                    if i > 0:
                        send_final(way, i, 1 - way)
                for way, source, _ in ways:
                    if i == 2:
                        relay[way, 2].wait_recv()
                    held = piece(source, i, way)
                    held[...] = held[...] + (rl1[way] if i == 2 else rl2[way, (p, o)[i]])
                    send_final(way, i, way)

    steps = (step0, step1, step2, step3, step4, step5)
    for t in range(len(steps) + len(chunks) - 1):
        for n in range(len(chunks)):
            if 0 <= t - n < len(steps):
                steps[t - n](n)

    def arrived(i, l):
        final[0, i, l].wait_recv()
        final[1, i, l].wait_recv()
        return piece(3, i, l)[...] + (final_slot(0, i, l)[...] + final_slot(1, i, l)[...])

    across = []
    for l in (0, 1):
        c2[3, p, l] = arrived(0, l)
        across.append(send(c2.at[3, p, l], zin.at[l], C, 18 + l, pair))
    for l in (0, 1):
        lanes = pl.ds(pl.multiple_of(o * HALF + l * L2, 128), L2)
        out[:, lanes] = at[o, :, l * L2 : (l + 1) * L2] - arrived(1, l)
    summed_over_pair(3)
    for l in (0, 1):
        first = HALF + l * L1
        out[:, HALF + first : HALF + first + L1] = at[o, :, first : first + L1] - arrived(2, l)
    for l in (0, 1):
        across[l].wait_recv()
        lanes = pl.ds(pl.multiple_of(p * HALF + l * L2, 128), L2)
        out[:, lanes] = at[p, :, l * L2 : (l + 1) * L2] - zin[l]

    for copy in sent:
        copy.wait_send()


def projected(raw, psi, table, panels, offsets):
    dma = pltpu.SemaphoreType.DMA
    vmem, hbm = pl.BlockSpec(memory_space=pltpu.VMEM), pl.BlockSpec(memory_space=pltpu.HBM)
    return pl.pallas_call(
        kernel,
        out_shape=jax.ShapeDtypeStruct((COLS, SLAB), F32),
        in_specs=[hbm] * 5,
        out_specs=vmem,
        scratch_shapes=[
            pltpu.VMEM((COLS, SLAB), F32),
            pltpu.VMEM((16, PANEL), F32),
            pltpu.SMEM((2,), jnp.int32),
            pltpu.SMEM((16,), jnp.int32),
            pltpu.VMEM((2, COLS, MINE), F32),
            pltpu.VMEM((2, MINE, BANDS), F32),
            pltpu.VMEM((2, HALF, BANDS), F32),
            pltpu.VMEM((4, 2, COLS, MINE), F32),
            pltpu.VMEM((1024, 2 * MINE), BF16),
            pltpu.VMEM((1024, 2 * MINE), BF16),
            pltpu.VMEM((2 * MINE, BANDS), BF16),
            pltpu.VMEM((2 * MINE, BANDS), BF16),
            pltpu.VMEM((2 * HALF, BANDS), BF16),
            pltpu.VMEM((2 * HALF, BANDS), BF16),
            pltpu.VMEM((16, BANDS), F32),
            pltpu.VMEM((2, 16, BANDS), F32),
            pltpu.VMEM((2, 1024, BANDS), F32),
            pltpu.VMEM((2, 1024, BANDS), F32),
            pltpu.VMEM((4, 2, 2, COLS, L2), F32),
            pltpu.VMEM((4, 2, 2, COLS, L1), F32),
            pltpu.VMEM((2, 512, BANDS), F32),
            pltpu.VMEM((5, 2, 3, 2, 16, BANDS), F32),
            pltpu.VMEM((5, 2, 3, 2, 16, BANDS), F32),
            pltpu.VMEM((5, 2, 2, 16, BANDS), F32),
            pltpu.VMEM((2, 2, COLS, L2), F32),
            pltpu.VMEM((2, COLS, L1), F32),
            pltpu.VMEM((2, 2, 2, COLS, L2), F32),
            pltpu.VMEM((2, 2, COLS, L1), F32),
            pltpu.VMEM((2, COLS, L2), F32),
            pltpu.VMEM((4, 2, COLS, L1), F32),
            dma((6,)), dma((8,)), dma((8,)), dma((5,)), dma((5,)),
            dma((100,)), dma((100,)), dma((24,)), dma((24,)),
        ],
        compiler_params=pltpu.CompilerParams(
            collective_id=0, has_side_effects=True, vmem_limit_bytes=52 * 1024 * 1024
        ),
    )(raw, psi, table, panels, offsets)


def turn_kernel(offsets, value, out):
    offset = offsets[lax.axis_index("ga")]
    for part in (0, 1):
        out[part] = pltpu.roll(value[part], offset, 1)


def turned_back(value, offsets):
    block = pl.BlockSpec((2, 16, SLAB), lambda k: (0, k, 0))
    return pl.pallas_call(
        turn_kernel,
        grid=(COLS // 2 // 16,),
        out_shape=jax.ShapeDtypeStruct((2, COLS // 2, SLAB), F32),
        in_specs=[pl.BlockSpec(memory_space=pltpu.SMEM), block],
        out_specs=block,
        compiler_params=pltpu.CompilerParams(vmem_limit_bytes=8 * 1024 * 1024),
    )(offsets, value)


def per_device(psi, dpsi, band_weight, panel_band, slab_offset):
    raw = jnp.swapaxes(dpsi, 1, 2).reshape(COLS, SLAB)
    result = projected(raw, psi, band_weight.reshape(-1, PANEL), panel_band, slab_offset)
    return jnp.swapaxes(turned_back(result.reshape(2, COLS // 2, SLAB), slab_offset), 1, 2)


def solution(mesh):
    in_specs = (P(None, "ga", "ba"), P(None, "ga", "ba"), P(), P("ba"), P())
    out_specs = P(None, "ga", "ba")
    return jax.shard_map(
        per_device, mesh=mesh, in_specs=in_specs, out_specs=out_specs, check_vma=False
    )
```

```python
import jax
import jax.numpy as jnp
from jax import lax
from jax.experimental import pallas as pl
from jax.experimental.pallas import tpu as pltpu
from jax.sharding import PartitionSpec as P

F32, BF16 = jnp.float32, jnp.bfloat16
PANEL = 128
SLAB = 2048
BANDS = 256
COLS = 128
HALF = 768
BOTH = SLAB - 2 * HALF
MINE = HALF + BOTH
PIECES = (0, 64, 256, 512, 640, HALF)
LAST = PIECES[-2]
L2, L1 = HALF // 2, BOTH // 2
NT = (((1,), (1,)), ((), ()))


def split(value):
    high = value.astype(BF16)
    return high, (value - high.astype(F32)).astype(BF16)


def three(dot, left, right):
    return dot(left[0], right[0]) + (dot(left[0], right[1]) + dot(left[1], right[0]))


def nn(left, right):
    return jnp.dot(left, right, preferred_element_type=F32)


def nt(left, right):
    return lax.dot_general(left, right, NT, preferred_element_type=F32)


def kernel(
    raw_hbm, psi, table_hbm, panels_hbm, offsets_hbm, out,
    raw, table, panels, offsets, at, psi_o, psi_p, a_v, a_hi, a_lo, o_hi, o_lo, p_hi, p_lo, ws, wv, m, w, c2, c1,
    r0, r1, r2, s, rl2, rl1, fin2, fin1, zin, zg,
    local_sem, a_s, a_r, p_s, p_r, g_s, g_r, c_s, c_r,
):
    ga, ba = lax.axis_index("ga"), lax.axis_index("ba")
    x, zhi, core = ga // 4, (ga // 2) % 2, ga % 2
    y, o = ba // 2, ba % 2
    p = 1 - o
    z = zhi * 2 + o
    oc = 1 - core

    def device(x=x, z=z, y=y, core=core):
        return (x * 4 + (z // 2) * 2 + core, y * 2 + z % 2)

    pair = device(z=zhi * 2 + p)
    up, down = device(y=(y + 1) % 4), device(y=(y + 3) % 4)
    other = device(core=oc)
    along_x = [device(x=(x + k) % 4) for k in (1, 2, 3)]
    along_z = [device(z=(z + k) % 4) for k in (1, 2, 3)]

    sent = []

    def send(src, dst, sems, index, to):
        copy = pltpu.make_async_remote_copy(
            src_ref=src, dst_ref=dst, send_sem=sems[0].at[index], recv_sem=sems[1].at[index],
            device_id=to, device_id_type=pl.DeviceIdType.MESH,
        )
        copy.start()
        sent.append(copy)
        return copy

    def half_at(which):
        return pl.multiple_of(which * HALF, HALF)

    barrier = pltpu.get_barrier_semaphore()
    peers = [up, down, other, *along_x, *along_z]
    for peer in peers:
        pl.semaphore_signal(barrier, inc=1, device_id=peer, device_id_type=pl.DeviceIdType.MESH)

    small = [
        pltpu.make_async_copy(offsets_hbm, offsets, local_sem.at[3]),
        pltpu.make_async_copy(table_hbm, table, local_sem.at[4]),
        pltpu.make_async_copy(panels_hbm, panels, local_sem.at[5]),
    ]
    local = [
        pltpu.make_async_copy(raw_hbm, raw, local_sem.at[0]),
        pltpu.make_async_copy(
            psi.at[:, pl.ds(half_at(o), HALF), :], psi_o.at[:, pl.ds(0, HALF), :], local_sem.at[1]
        ),
        pltpu.make_async_copy(
            psi.at[:, pl.ds(2 * HALF, BOTH), :], psi_o.at[:, pl.ds(HALF, BOTH), :], local_sem.at[2]
        ),
    ]
    for copy in small + local:
        copy.start()

    waves = []

    def send_waves(k):
        first, count = PIECES[k], PIECES[k + 1] - PIECES[k]
        waves.append(
            send(
                psi.at[:, pl.ds(pl.multiple_of(p * HALF + first, 64), count), :],
                psi_p.at[:, pl.ds(first, count), :], (p_s, p_r), k, pair,
            )
        )

    pl.semaphore_wait(barrier, len(peers))
    send_waves(0)
    for copy in small:
        copy.wait()
    local[0].wait()

    offset = offsets[ga]
    lane = lax.broadcasted_iota(jnp.int32, (16, 128), 1)

    def align(k, _):
        rows = pl.ds(pl.multiple_of(k * 16, 16), 16)
        tiles = [raw[rows, t * 128 : (t + 1) * 128] for t in range(16)]
        for bit in (10, 9, 8, 7, 6, 5, 4, 3, 2, 1, 0):
            turn = jnp.full((16, 128), (offset >> bit) & 1, jnp.int32) != 0
            if bit >= 7:
                moved = [tiles[(t + (1 << (bit - 7))) % 16] for t in range(16)]
            else:
                rolled = [pltpu.roll(tile, 128 - (1 << bit), 1) for tile in tiles]
                inside = lane < 128 - (1 << bit)
                moved = [jnp.where(inside, rolled[t], rolled[(t + 1) % 16]) for t in range(16)]
            tiles = [jnp.where(turn, new, old) for new, old in zip(moved, tiles)]
        for t, value in enumerate(tiles):
            if t * 128 < 2 * HALF:
                half, first = divmod(t * 128, HALF)
                at[half, rows, first : first + 128] = value
            else:
                first = t * 128 - HALF
                at[0, rows, first : first + 128] = value
                at[1, rows, first : first + 128] = value
        return 0

    lax.fori_loop(0, COLS // 16, align, 0)

    row = lax.broadcasted_iota(jnp.int32, (16, PANEL), 0)
    for k in (0, 1):
        chosen = jnp.where(row == jnp.full((16, PANEL), panels[k], jnp.int32), table[...], 0.0)
        ws[:, k * PANEL : (k + 1) * PANEL] = jnp.broadcast_to(
            jnp.sum(chosen, axis=0, keepdims=True), (32, PANEL)
        )
    wv[o] = ws[...]

    A = (a_s, a_r)
    lanes = (pl.ds(0, MINE // 2), pl.ds(MINE // 2, MINE // 2))
    a_pair = [send(at.at[p, :, l], a_v.at[3, o, :, l], A, i, pair) for i, l in enumerate(lanes)]
    ring = ((0, up, 2), (1, down, 1))

    def pass_on(source, half, base):
        return {
            (way, i): send(source.at[:, lanes[i]], a_v.at[slot, half, :, lanes[i]], A, base + way * 2 + i, to)
            for order in (0, 1) for way, to, slot in ring for i in (way ^ order,)
        }

    def forward(half, base):
        return [
            send(a_v.at[slot, half, :, lanes[way]], a_v.at[0, half, :, lanes[way]], A, base + way, to)
            for way, to, slot in ring
        ]

    near_o = pass_on(at.at[o], o, 2)
    w_pair = send(ws, wv.at[o], A, 14, pair)
    for k in range(1, len(PIECES) - 1):
        send_waves(k)

    def keep_columns(value, rel, half):
        rows = rel * 256 + half * COLS
        top = pl.ds(pl.multiple_of(rows, 64), 64)
        bottom = pl.ds(pl.multiple_of(rows + 64, 64), 64)
        for ref, part in zip((a_hi, a_lo), split(value)):
            ref[top, :MINE] = part[:64]
            ref[bottom, :MINE] = part[64:]
            ref[top, MINE:] = part[64:]
            ref[bottom, MINE:] = -part[:64]

    def keep_waves(ref, high_ref, low_ref, length, first, count):
        for part in (0, 1):
            high, low = split(ref[part, first : first + count, :])
            high_ref[part * length + first : part * length + first + count, :] = high
            low_ref[part * length + first : part * length + first + count, :] = low

    def keep_piece(k):
        waves[k].wait_recv()
        keep_waves(psi_p, p_hi, p_lo, HALF, PIECES[k], PIECES[k + 1] - PIECES[k])

    keep_columns(at[o], 3, o)
    local[1].wait()
    local[2].wait()
    keep_waves(psi_o, o_hi, o_lo, MINE, 0, MINE)
    keep_piece(0)

    for way in (0, 1):
        near_o[way, way].wait_recv()
    far_o = forward(o, 10)
    a_pair[0].wait_recv()
    a_pair[1].wait_recv()
    near_p = pass_on(a_v.at[3, p], p, 6)
    keep_columns(a_v[3, p], 3, p)
    for way, _, slot in ring:
        near_o[way, 1 - way].wait_recv()
        keep_columns(a_v[slot, o], slot, o)
    keep_piece(1)
    for way in (0, 1):
        near_p[way, way].wait_recv()
    far_p = forward(p, 12)
    for copy in far_o:
        copy.wait_recv()
    keep_columns(a_v[0, o], 0, o)
    keep_piece(2)
    for way, _, slot in ring:
        near_p[way, 1 - way].wait_recv()
        keep_columns(a_v[slot, p], slot, p)
    w_pair.wait_recv()

    def own_bands(rel):
        rows = pl.ds(pl.multiple_of(rel * 256, 256), 256)
        m[o, rows, :] = three(nn, (a_hi[rows, :], a_lo[rows, :]), (o_hi[...], o_lo[...]))

    def block_rows(rel):
        return pl.ds(pl.multiple_of(rel * 256, 256), 256)

    def pair_bands(rows, first, last):
        total = None
        for part in (0, 1):
            ks, rs = pl.ds(part * MINE + first, last - first), pl.ds(part * HALF + first, last - first)
            term = three(nn, (a_hi[rows, ks], a_lo[rows, ks]), (p_hi[rs, :], p_lo[rs, :]))
            total = term if total is None else total + term
        return rows, total

    def early(rel, _):
        own_bands(rel)
        rows, total = pair_bands(block_rows(rel), 0, PIECES[3])
        m[p, rows, :] = total
        return 0

    lax.fori_loop(1, 4, early, 0)
    for copy in far_p:
        copy.wait_recv()
    keep_columns(a_v[0, p], 0, p)
    lax.fori_loop(0, 1, early, 0)
    keep_piece(3)

    def later(rel, _):
        rows, total = pair_bands(block_rows(rel), PIECES[3], LAST)
        m[p, rows, :] = m[p, rows, :] + total
        return 0

    lax.fori_loop(0, 4, later, 0)
    keep_piece(4)

    G = (g_s, g_r)
    chunks = ((0, 256), (256, 512), (768, 256))
    flight = {}

    def quarter(n, part, q):
        first, length = chunks[n]
        return pl.ds(
            pl.multiple_of(first + (core * 2 + part) * (length // 4) + q * (length // 16), 8),
            length // 16,
        )

    def core_rows(n, which):
        first, length = chunks[n]
        return pl.ds(pl.multiple_of(first + which * (length // 2), 64), length // 2)

    def landed(n):
        for copy in flight[n]:
            copy.wait_recv()
        flight[n] = []

    def step0(n):
        first, length = chunks[n]
        rows, total = pair_bands(pl.ds(first, length), LAST, HALF)
        m[p, rows, :] = m[p, rows, :] + total
        to = r0.at[:, pl.ds(first // 2, length // 2), :]
        flight[n] = [send(m.at[:, core_rows(n, oc), :], to, G, n * 20, other)]

    def step1(n):
        landed(n)
        first, length = chunks[n]
        rows = core_rows(n, core)
        m[:, rows, :] = m[:, rows, :] + r0[:, first // 2 : (first + length) // 2, :]
        few = pl.ds(0, length // 16)
        for k in (1, 2, 3):
            to_x, to_z = (x + k) % 4, (z + k) % 4
            flight[n] += [
                send(m.at[:, quarter(n, 0, to_x), :], r1.at[n, 0, k - 1, :, few], G, n * 20 + k, along_x[k - 1]),
                send(m.at[:, quarter(n, 1, to_z), :], r1.at[n, 1, k - 1, :, few], G, n * 20 + 3 + k, along_z[k - 1]),
            ]

    def four(mine, ref, n, part):
        few = chunks[n][1] // 16
        return (mine + ref[n, part, 0, :, :few]) + (ref[n, part, 1, :, :few] + ref[n, part, 2, :, :few])

    def step2(n):
        landed(n)
        few = pl.ds(0, chunks[n][1] // 16)
        for part, q in ((0, x), (1, z)):
            s[n, part, :, few, :] = four(m[:, quarter(n, part, q), :], r1, n, part)
        for k in (1, 2, 3):
            flight[n] += [
                send(s.at[n, 0, :, few], r2.at[n, 0, k - 1, :, few], G, n * 20 + 6 + k, along_z[k - 1]),
                send(s.at[n, 1, :, few], r2.at[n, 1, k - 1, :, few], G, n * 20 + 9 + k, along_x[k - 1]),
            ]

    def step3(n):
        landed(n)
        few = chunks[n][1] // 16
        for part, q in ((0, x), (1, z)):
            w[:, quarter(n, part, q), :] = four(s[n, part, :, :few], r2, n, part) * wv[:, :few, :]
        for_x, for_z = w.at[:, quarter(n, 0, x), :], w.at[:, quarter(n, 1, z), :]
        for k in (1, 2, 3):
            flight[n] += [
                send(for_x, for_x, G, n * 20 + 12 + k, along_x[k - 1]),
                send(for_z, for_z, G, n * 20 + 15 + k, along_z[k - 1]),
            ]

    def step4(n):
        landed(n)
        block = w.at[:, core_rows(n, core), :]
        flight[n] = [send(block, block, G, n * 20 + 19, other)]

    C = (c_s, c_r)
    pairs = {}

    def corrections(rel):
        left = []
        for half in (o, p):
            plain = split(w[half, rel * 256 : rel * 256 + 256, :])
            left.append((plain, [
                jnp.concatenate([-v[64:128], v[:64], -v[192:], v[128:192]], axis=0) for v in plain
            ]))
        mine, theirs = left

        def both(l):
            total = None
            for imag in (0, 1):
                rows = pl.ds(imag * MINE + HALF + l * L1, L1)
                term = three(nt, mine[imag], (o_hi[rows, :], o_lo[rows, :]))
                total = term if total is None else total + term
            c1[rel, 0, l] = total[:COLS]
            c1[rel, 1, l] = total[COLS:]

        def alone(l):
            total = None
            for imag in (0, 1):
                rows = pl.ds(imag * MINE + l * L2, L2)
                term = three(nt, mine[imag], (o_hi[rows, :], o_lo[rows, :]))
                total = term if total is None else total + term
                rows = pl.ds(imag * HALF + l * L2, L2)
                total = total + three(nt, theirs[imag], (p_hi[rows, :], p_lo[rows, :]))
            c2[rel, 0, l] = total[:COLS]
            c2[rel, 1, l] = total[COLS:]

        return both, alone

    ways = ((0, 1, up), (1, 2, down))
    relay, final = {}, {}

    def piece(rel, i, l):
        return (c2.at[rel, p, l], c2.at[rel, o, l], c1.at[rel, o, l])[i]

    def summed_over_pair(rel):
        pairs[rel].wait_recv()
        c1[rel, o] = c1[rel, o] + zg[rel]

    def final_slot(way, i, l):
        return fin1.at[way, l] if i == 2 else fin2.at[way, i, l]

    def send_final(way, i, l):
        _, rel, to = ways[way]
        final[way, i, l] = send(
            piece(rel, i, l), final_slot(way, i, l), C, 6 + way * 6 + i * 2 + l, to
        )

    def to_pair(rel):
        pairs[rel] = send(c1.at[rel, p], zg.at[rel], C, 20 + rel, pair)

    def send_relay(i):
        for way, _, to in ways:
            slot = rl1.at[way] if i == 2 else rl2.at[way, i]
            relay[way, i] = send(piece(0, i, way), slot, C, way * 3 + i, to)

    def send_held(way, i):
        relay[way, i].wait_recv()
        held = piece(ways[way][1], i, way)
        held[...] = held[...] + (rl1[way] if i == 2 else rl2[way, i])
        send_final(way, i, way)

    def step5(n):
        landed(n)
        if n == 0:
            both, alone = corrections(0)
            alone(0)
            alone(1)
            send_relay(0)
            send_relay(1)
            both(0)
            both(1)
            to_pair(0)
        elif n == 1:
            for way, rel, _ in ways:
                both, alone = corrections(rel)
                both(0)
                both(1)
                to_pair(rel)
                alone(1 - way)
                send_final(way, 0, 1 - way)
                alone(way)
            summed_over_pair(0)
            send_relay(2)
            for i in (0, 1):
                for way in (0, 1):
                    if i > 0:
                        send_final(way, i, 1 - way)
                for way in (0, 1):
                    send_held(way, i)
        else:
            both, alone = corrections(3)
            both(0)
            both(1)
            to_pair(3)
            for way, rel, _ in ways:
                summed_over_pair(rel)
                send_final(way, 2, 1 - way)
            for way in (0, 1):
                send_held(way, 2)
            alone(0)
            alone(1)

    steps = (step0, step1, step2, step3, step4, step5)
    for t in range(len(steps) + len(chunks) - 1):
        for n in range(len(chunks)):
            if 0 <= t - n < len(steps):
                steps[t - n](n)

    def arrived(i, l):
        final[0, i, l].wait_recv()
        final[1, i, l].wait_recv()
        return piece(3, i, l)[...] + (final_slot(0, i, l)[...] + final_slot(1, i, l)[...])

    across = []
    for l in (0, 1):
        c2[3, p, l] = arrived(0, l)
        across.append(send(c2.at[3, p, l], zin.at[l], C, 18 + l, pair))
    for l in (0, 1):
        lanes = pl.ds(pl.multiple_of(o * HALF + l * L2, 128), L2)
        out[:, lanes] = at[o, :, l * L2 : (l + 1) * L2] - arrived(1, l)
    summed_over_pair(3)
    for l in (0, 1):
        first = HALF + l * L1
        out[:, HALF + first : HALF + first + L1] = at[o, :, first : first + L1] - arrived(2, l)
    for l in (0, 1):
        across[l].wait_recv()
        lanes = pl.ds(pl.multiple_of(p * HALF + l * L2, 128), L2)
        out[:, lanes] = at[p, :, l * L2 : (l + 1) * L2] - zin[l]

    for copy in sent:
        copy.wait_send()


def projected(raw, psi, table, panels, offsets):
    dma = pltpu.SemaphoreType.DMA
    vmem, hbm = pl.BlockSpec(memory_space=pltpu.VMEM), pl.BlockSpec(memory_space=pltpu.HBM)
    return pl.pallas_call(
        kernel,
        out_shape=jax.ShapeDtypeStruct((COLS, SLAB), F32),
        in_specs=[hbm] * 5,
        out_specs=vmem,
        scratch_shapes=[
            pltpu.VMEM((COLS, SLAB), F32),
            pltpu.VMEM((16, PANEL), F32),
            pltpu.SMEM((2,), jnp.int32),
            pltpu.SMEM((16,), jnp.int32),
            pltpu.VMEM((2, COLS, MINE), F32),
            pltpu.VMEM((2, MINE, BANDS), F32),
            pltpu.VMEM((2, HALF, BANDS), F32),
            pltpu.VMEM((4, 2, COLS, MINE), F32),
            pltpu.VMEM((1024, 2 * MINE), BF16),
            pltpu.VMEM((1024, 2 * MINE), BF16),
            pltpu.VMEM((2 * MINE, BANDS), BF16),
            pltpu.VMEM((2 * MINE, BANDS), BF16),
            pltpu.VMEM((2 * HALF, BANDS), BF16),
            pltpu.VMEM((2 * HALF, BANDS), BF16),
            pltpu.VMEM((32, BANDS), F32),
            pltpu.VMEM((2, 32, BANDS), F32),
            pltpu.VMEM((2, 1024, BANDS), F32),
            pltpu.VMEM((2, 1024, BANDS), F32),
            pltpu.VMEM((4, 2, 2, COLS, L2), F32),
            pltpu.VMEM((4, 2, 2, COLS, L1), F32),
            pltpu.VMEM((2, 512, BANDS), F32),
            pltpu.VMEM((3, 2, 3, 2, 32, BANDS), F32),
            pltpu.VMEM((3, 2, 3, 2, 32, BANDS), F32),
            pltpu.VMEM((3, 2, 2, 32, BANDS), F32),
            pltpu.VMEM((2, 2, COLS, L2), F32),
            pltpu.VMEM((2, COLS, L1), F32),
            pltpu.VMEM((2, 2, 2, COLS, L2), F32),
            pltpu.VMEM((2, 2, COLS, L1), F32),
            pltpu.VMEM((2, COLS, L2), F32),
            pltpu.VMEM((4, 2, COLS, L1), F32),
            dma((6,)), dma((15,)), dma((15,)), dma((5,)), dma((5,)),
            dma((60,)), dma((60,)), dma((24,)), dma((24,)),
        ],
        compiler_params=pltpu.CompilerParams(
            collective_id=0, has_side_effects=True, vmem_limit_bytes=62 * 1024 * 1024
        ),
    )(raw, psi, table, panels, offsets)


def turn_kernel(offsets, value, out):
    offset = offsets[lax.axis_index("ga")]
    for part in (0, 1):
        out[part] = pltpu.roll(value[part], offset, 1)


def turned_back(value, offsets):
    block = pl.BlockSpec((2, 16, SLAB), lambda k: (0, k, 0))
    return pl.pallas_call(
        turn_kernel,
        grid=(COLS // 2 // 16,),
        out_shape=jax.ShapeDtypeStruct((2, COLS // 2, SLAB), F32),
        in_specs=[pl.BlockSpec(memory_space=pltpu.SMEM), block],
        out_specs=block,
        compiler_params=pltpu.CompilerParams(vmem_limit_bytes=62 * 1024 * 1024),
    )(offsets, value)


def per_device(psi, dpsi, band_weight, panel_band, slab_offset):
    raw = jnp.swapaxes(dpsi, 1, 2).reshape(COLS, SLAB)
    result = projected(raw, psi, band_weight.reshape(-1, PANEL), panel_band, slab_offset)
    return jnp.swapaxes(turned_back(result.reshape(2, COLS // 2, SLAB), slab_offset), 1, 2)


def solution(mesh):
    in_specs = (P(None, "ga", "ba"), P(None, "ga", "ba"), P(), P("ba"), P())
    out_specs = P(None, "ga", "ba")
    return jax.shard_map(
        per_device, mesh=mesh, in_specs=in_specs, out_specs=out_specs, check_vma=False
    )
```

```python
import jax
import jax.numpy as jnp
from jax import lax
from jax.experimental import pallas as pl
from jax.experimental.pallas import tpu as pltpu
from jax.sharding import PartitionSpec as P

F32, BF16 = jnp.float32, jnp.bfloat16
PANEL = 128
SLAB = 2048
BANDS = 256
COLS = 128
HALF = 768
BOTH = SLAB - 2 * HALF
MINE = HALF + BOTH
PIECES = (0, 64, 256, 512, 640, HALF)
LAST = PIECES[-2]
L2, L1 = HALF // 2, BOTH // 2
ORDER = (
    (0, 0), (1, 0), (0, 1), (2, 0), (1, 1), (0, 2), (3, 0), (2, 1), (1, 2), (4, 0), (3, 1), (2, 2),
    (5, 0), (4, 1), (6, 0), (3, 2), (5, 1), (4, 2), (5, 2),
)
NT = (((1,), (1,)), ((), ()))


def split(value):
    high = value.astype(BF16)
    return high, (value - high.astype(F32)).astype(BF16)


def three(dot, left, right):
    return dot(left[0], right[0]) + (dot(left[0], right[1]) + dot(left[1], right[0]))


def nn(left, right):
    return jnp.dot(left, right, preferred_element_type=F32)


def nt(left, right):
    return lax.dot_general(left, right, NT, preferred_element_type=F32)


def kernel(
    raw_hbm, psi, table_hbm, panels_hbm, offsets_hbm, out,
    raw, table, panels, offsets, out_v, at, psi_o, psi_p, a_v, a_hi, a_lo, o_hi, o_lo, p_hi, p_lo, ws, wv, m, w, c2, c1,
    r0, r1, r2, s, rl2, rl1, fin2, fin1, zin, zg,
    local_sem, a_s, a_r, p_s, p_r, g_s, g_r, c_s, c_r,
):
    ga, ba = lax.axis_index("ga"), lax.axis_index("ba")
    x, zhi, core = ga // 4, (ga // 2) % 2, ga % 2
    y, o = ba // 2, ba % 2
    p = 1 - o
    z = zhi * 2 + o
    oc = 1 - core

    def device(x=x, z=z, y=y, core=core):
        return (x * 4 + (z // 2) * 2 + core, y * 2 + z % 2)

    pair = device(z=zhi * 2 + p)
    up, down = device(y=(y + 1) % 4), device(y=(y + 3) % 4)
    other = device(core=oc)
    along_x = [device(x=(x + k) % 4) for k in (1, 2, 3)]
    along_z = [device(z=(z + k) % 4) for k in (1, 2, 3)]

    sent = []

    def send(src, dst, sems, index, to):
        copy = pltpu.make_async_remote_copy(
            src_ref=src, dst_ref=dst, send_sem=sems[0].at[index], recv_sem=sems[1].at[index],
            device_id=to, device_id_type=pl.DeviceIdType.MESH,
        )
        copy.start()
        sent.append(copy)
        return copy

    def half_at(which):
        return pl.multiple_of(which * HALF, HALF)

    barrier = pltpu.get_barrier_semaphore()
    peers = [up, down, other, *along_x, *along_z]
    for peer in peers:
        pl.semaphore_signal(barrier, inc=1, device_id=peer, device_id_type=pl.DeviceIdType.MESH)

    small = [
        pltpu.make_async_copy(offsets_hbm, offsets, local_sem.at[3]),
        pltpu.make_async_copy(table_hbm, table, local_sem.at[4]),
        pltpu.make_async_copy(panels_hbm, panels, local_sem.at[5]),
    ]
    local = [
        pltpu.make_async_copy(raw_hbm, raw, local_sem.at[0]),
        pltpu.make_async_copy(
            psi.at[:, pl.ds(half_at(o), HALF), :], psi_o.at[:, pl.ds(0, HALF), :], local_sem.at[1]
        ),
        pltpu.make_async_copy(
            psi.at[:, pl.ds(2 * HALF, BOTH), :], psi_o.at[:, pl.ds(HALF, BOTH), :], local_sem.at[2]
        ),
    ]
    for copy in small + local:
        copy.start()

    waves = []

    def send_waves(k):
        first, count = PIECES[k], PIECES[k + 1] - PIECES[k]
        waves.append(
            send(
                psi.at[:, pl.ds(pl.multiple_of(p * HALF + first, 64), count), :],
                psi_p.at[:, pl.ds(first, count), :], (p_s, p_r), k, pair,
            )
        )

    pl.semaphore_wait(barrier, len(peers))
    send_waves(0)
    for copy in small:
        copy.wait()
    local[0].wait()

    offset = offsets[ga]
    lane = lax.broadcasted_iota(jnp.int32, (16, 128), 1)

    def align(k, _):
        rows = pl.ds(pl.multiple_of(k * 16, 16), 16)
        tiles = [raw[rows, t * 128 : (t + 1) * 128] for t in range(16)]
        for bit in (10, 9, 8, 7, 6, 5, 4, 3, 2, 1, 0):
            turn = jnp.full((16, 128), (offset >> bit) & 1, jnp.int32) != 0
            if bit >= 7:
                moved = [tiles[(t + (1 << (bit - 7))) % 16] for t in range(16)]
            else:
                rolled = [pltpu.roll(tile, 128 - (1 << bit), 1) for tile in tiles]
                inside = lane < 128 - (1 << bit)
                moved = [jnp.where(inside, rolled[t], rolled[(t + 1) % 16]) for t in range(16)]
            tiles = [jnp.where(turn, new, old) for new, old in zip(moved, tiles)]
        for t, value in enumerate(tiles):
            if t * 128 < 2 * HALF:
                half, first = divmod(t * 128, HALF)
                at[half, rows, first : first + 128] = value
            else:
                first = t * 128 - HALF
                at[0, rows, first : first + 128] = value
                at[1, rows, first : first + 128] = value
        return 0

    lax.fori_loop(0, COLS // 16, align, 0)

    row = lax.broadcasted_iota(jnp.int32, (16, PANEL), 0)
    for k in (0, 1):
        chosen = jnp.where(row == jnp.full((16, PANEL), panels[k], jnp.int32), table[...], 0.0)
        ws[:, k * PANEL : (k + 1) * PANEL] = jnp.broadcast_to(
            jnp.sum(chosen, axis=0, keepdims=True), (32, PANEL)
        )
    wv[o] = ws[...]

    A = (a_s, a_r)
    lanes = (pl.ds(0, MINE // 2), pl.ds(MINE // 2, MINE // 2))
    a_pair = [send(at.at[p, :, l], a_v.at[3, o, :, l], A, i, pair) for i, l in enumerate(lanes)]
    ring = ((0, up, 2), (1, down, 1))

    def pass_on(source, half, base):
        return {
            (way, i): send(source.at[:, lanes[i]], a_v.at[slot, half, :, lanes[i]], A, base + way * 2 + i, to)
            for order in (0, 1) for way, to, slot in ring for i in (way ^ order,)
        }

    def forward(half, base):
        return [
            send(a_v.at[slot, half, :, lanes[way]], a_v.at[0, half, :, lanes[way]], A, base + way, to)
            for way, to, slot in ring
        ]

    near_o = pass_on(at.at[o], o, 2)
    w_pair = send(ws, wv.at[o], A, 14, pair)
    for k in range(1, len(PIECES) - 1):
        send_waves(k)

    def keep_columns(value, rel, half):
        rows = rel * 256 + half * COLS
        top = pl.ds(pl.multiple_of(rows, 64), 64)
        bottom = pl.ds(pl.multiple_of(rows + 64, 64), 64)
        for ref, part in zip((a_hi, a_lo), split(value)):
            ref[top, :MINE] = part[:64]
            ref[bottom, :MINE] = part[64:]
            ref[top, MINE:] = part[64:]
            ref[bottom, MINE:] = -part[:64]

    def keep_waves(ref, high_ref, low_ref, length, first, count):
        for part in (0, 1):
            high, low = split(ref[part, first : first + count, :])
            high_ref[part * length + first : part * length + first + count, :] = high
            low_ref[part * length + first : part * length + first + count, :] = low

    def keep_piece(k):
        waves[k].wait_recv()
        keep_waves(psi_p, p_hi, p_lo, HALF, PIECES[k], PIECES[k + 1] - PIECES[k])

    keep_columns(at[o], 3, o)
    local[1].wait()
    local[2].wait()
    keep_waves(psi_o, o_hi, o_lo, MINE, 0, MINE)
    keep_piece(0)

    for way in (0, 1):
        near_o[way, way].wait_recv()
    far_o = forward(o, 10)
    a_pair[0].wait_recv()
    a_pair[1].wait_recv()
    near_p = pass_on(a_v.at[3, p], p, 6)
    keep_columns(a_v[3, p], 3, p)
    for way, _, slot in ring:
        near_o[way, 1 - way].wait_recv()
        keep_columns(a_v[slot, o], slot, o)
    keep_piece(1)
    for way in (0, 1):
        near_p[way, way].wait_recv()
    far_p = forward(p, 12)
    for copy in far_o:
        copy.wait_recv()
    keep_columns(a_v[0, o], 0, o)
    keep_piece(2)
    for way, _, slot in ring:
        near_p[way, 1 - way].wait_recv()
        keep_columns(a_v[slot, p], slot, p)
    w_pair.wait_recv()

    def own_bands(rel):
        rows = pl.ds(pl.multiple_of(rel * 256, 256), 256)
        m[o, rows, :] = three(nn, (a_hi[rows, :], a_lo[rows, :]), (o_hi[...], o_lo[...]))

    def block_rows(rel):
        return pl.ds(pl.multiple_of(rel * 256, 256), 256)

    def pair_bands(rows, first, last):
        total = None
        for part in (0, 1):
            ks, rs = pl.ds(part * MINE + first, last - first), pl.ds(part * HALF + first, last - first)
            term = three(nn, (a_hi[rows, ks], a_lo[rows, ks]), (p_hi[rs, :], p_lo[rs, :]))
            total = term if total is None else total + term
        return rows, total

    keep_piece(3)

    def early(rel, _):
        own_bands(rel)
        rows, total = pair_bands(block_rows(rel), 0, LAST)
        m[p, rows, :] = total
        return 0

    lax.fori_loop(1, 4, early, 0)
    for copy in far_p:
        copy.wait_recv()
    keep_columns(a_v[0, p], 0, p)
    lax.fori_loop(0, 1, early, 0)
    keep_piece(4)

    G = (g_s, g_r)
    chunks = ((0, 256), (256, 512), (768, 256))
    flight = {}

    def quarter(n, part, q):
        first, length = chunks[n]
        return pl.ds(
            pl.multiple_of(first + (core * 2 + part) * (length // 4) + q * (length // 16), 8),
            length // 16,
        )

    def core_rows(n, which):
        first, length = chunks[n]
        return pl.ds(pl.multiple_of(first + which * (length // 2), 64), length // 2)

    def landed(n):
        for copy in flight[n]:
            copy.wait_recv()
        flight[n] = []

    def step0(n):
        first, length = chunks[n]
        rows, total = pair_bands(pl.ds(first, length), LAST, HALF)
        m[p, rows, :] = m[p, rows, :] + total
        to = r0.at[:, pl.ds(first // 2, length // 2), :]
        flight[n] = [send(m.at[:, core_rows(n, oc), :], to, G, n * 20, other)]

    def step1(n):
        landed(n)
        first, length = chunks[n]
        rows = core_rows(n, core)
        m[:, rows, :] = m[:, rows, :] + r0[:, first // 2 : (first + length) // 2, :]
        few = pl.ds(0, length // 16)
        for k in (1, 2, 3):
            to_x, to_z = (x + k) % 4, (z + k) % 4
            flight[n] += [
                send(m.at[:, quarter(n, 0, to_x), :], r1.at[n, 0, k - 1, :, few], G, n * 20 + k, along_x[k - 1]),
                send(m.at[:, quarter(n, 1, to_z), :], r1.at[n, 1, k - 1, :, few], G, n * 20 + 3 + k, along_z[k - 1]),
            ]

    def four(mine, ref, n, part):
        few = chunks[n][1] // 16
        return (mine + ref[n, part, 0, :, :few]) + (ref[n, part, 1, :, :few] + ref[n, part, 2, :, :few])

    def step2(n):
        landed(n)
        few = pl.ds(0, chunks[n][1] // 16)
        for part, q in ((0, x), (1, z)):
            s[n, part, :, few, :] = four(m[:, quarter(n, part, q), :], r1, n, part)
        for k in (1, 2, 3):
            flight[n] += [
                send(s.at[n, 0, :, few], r2.at[n, 0, k - 1, :, few], G, n * 20 + 6 + k, along_z[k - 1]),
                send(s.at[n, 1, :, few], r2.at[n, 1, k - 1, :, few], G, n * 20 + 9 + k, along_x[k - 1]),
            ]

    def step3(n):
        landed(n)
        few = chunks[n][1] // 16
        for part, q in ((0, x), (1, z)):
            w[:, quarter(n, part, q), :] = four(s[n, part, :, :few], r2, n, part) * wv[:, :few, :]
        for_x, for_z = w.at[:, quarter(n, 0, x), :], w.at[:, quarter(n, 1, z), :]
        for k in (1, 2, 3):
            flight[n] += [
                send(for_x, for_x, G, n * 20 + 12 + k, along_x[k - 1]),
                send(for_z, for_z, G, n * 20 + 15 + k, along_z[k - 1]),
            ]

    def step4(n):
        landed(n)
        block = w.at[:, core_rows(n, core), :]
        flight[n] = [send(block, block, G, n * 20 + 19, other)]

    C = (c_s, c_r)
    pairs = {}

    def corrections(rel):
        left = []
        for half in (o, p):
            plain = split(w[half, rel * 256 : rel * 256 + 256, :])
            left.append((plain, [
                jnp.concatenate([-v[64:128], v[:64], -v[192:], v[128:192]], axis=0) for v in plain
            ]))
        mine, theirs = left

        def both(l):
            total = None
            for imag in (0, 1):
                rows = pl.ds(imag * MINE + HALF + l * L1, L1)
                term = three(nt, mine[imag], (o_hi[rows, :], o_lo[rows, :]))
                total = term if total is None else total + term
            c1[rel, 0, l] = total[:COLS]
            c1[rel, 1, l] = total[COLS:]

        def alone(l):
            total = None
            for imag in (0, 1):
                rows = pl.ds(imag * MINE + l * L2, L2)
                term = three(nt, mine[imag], (o_hi[rows, :], o_lo[rows, :]))
                total = term if total is None else total + term
                rows = pl.ds(imag * HALF + l * L2, L2)
                total = total + three(nt, theirs[imag], (p_hi[rows, :], p_lo[rows, :]))
            c2[rel, 0, l] = total[:COLS]
            c2[rel, 1, l] = total[COLS:]

        return both, alone

    ways = ((0, 1, up), (1, 2, down))
    relay, final = {}, {}

    def piece(rel, i, l):
        return (c2.at[rel, p, l], c2.at[rel, o, l], c1.at[rel, o, l])[i]

    def summed_over_pair(rel):
        pairs[rel].wait_recv()
        c1[rel, o] = c1[rel, o] + zg[rel]

    def final_slot(way, i, l):
        return fin1.at[way, l] if i == 2 else fin2.at[way, i, l]

    def send_final(way, i, l):
        _, rel, to = ways[way]
        final[way, i, l] = send(
            piece(rel, i, l), final_slot(way, i, l), C, 6 + way * 6 + i * 2 + l, to
        )

    def to_pair(rel):
        pairs[rel] = send(c1.at[rel, p], zg.at[rel], C, 20 + rel, pair)

    def send_relay(i):
        for way, _, to in ways:
            slot = rl1.at[way] if i == 2 else rl2.at[way, i]
            relay[way, i] = send(piece(0, i, way), slot, C, way * 3 + i, to)

    def send_held(way, i):
        relay[way, i].wait_recv()
        held = piece(ways[way][1], i, way)
        held[...] = held[...] + (rl1[way] if i == 2 else rl2[way, i])
        send_final(way, i, way)

    def step5(n):
        landed(n)
        if n == 0:
            _, alone = corrections(0)
            for way, _, to in ways:
                alone(way)
                for i in (0, 1):
                    relay[way, i] = send(piece(0, i, way), rl2.at[way, i], C, way * 3 + i, to)
        elif n == 1:
            work = {rel: corrections(rel) for _, rel, _ in ways}
            for way, rel, _ in ways:
                work[rel][1](1 - way)
                send_final(way, 0, 1 - way)
            for way, rel, _ in ways:
                work[rel][1](way)
                send_held(way, 0)
            for way in (0, 1):
                send_final(way, 1, 1 - way)
            for way in (0, 1):
                send_held(way, 1)
            summed_over_pair(0)
            send_relay(2)
            for _, rel, _ in ways:
                both, _ = work[rel]
                both(0)
                both(1)
                to_pair(rel)
        else:
            both, alone = corrections(3)
            both(0)
            both(1)
            to_pair(3)
            alone(0)
            alone(1)
            for way, rel, _ in ways:
                summed_over_pair(rel)
                send_final(way, 2, 1 - way)
            for way in (0, 1):
                send_held(way, 2)

    def step6(n):
        if n == 0:
            both, _ = corrections(0)
            both(0)
            both(1)
            to_pair(0)

    steps = (step0, step1, step2, step3, step4, step5, step6)
    for step, n in ORDER:
        steps[step](n)

    def arrived(i, l):
        final[0, i, l].wait_recv()
        final[1, i, l].wait_recv()
        return piece(3, i, l)[...] + (final_slot(0, i, l)[...] + final_slot(1, i, l)[...])

    across, written = [], []

    def write(first, length, value):
        lanes = pl.ds(first, length)
        out_v[:, lanes] = value
        copy = pltpu.make_async_copy(out_v.at[:, lanes], out.at[:, lanes], local_sem.at[6 + len(written)])
        copy.start()
        written.append(copy)

    for l in (0, 1):
        c2[3, p, l] = arrived(0, l)
        across.append(send(c2.at[3, p, l], zin.at[l], C, 18 + l, pair))
    for l in (0, 1):
        value = at[o, :, l * L2 : (l + 1) * L2] - arrived(1, l)
        write(pl.multiple_of(o * HALF + l * L2, 128), L2, value)
    for l in (0, 1):
        across[l].wait_recv()
        value = at[p, :, l * L2 : (l + 1) * L2] - zin[l]
        write(pl.multiple_of(p * HALF + l * L2, 128), L2, value)
    summed_over_pair(3)
    for l in (0, 1):
        first = HALF + l * L1
        value = at[o, :, first : first + L1] - arrived(2, l)
        write(HALF + first, L1, value)

    for copy in written:
        copy.wait()
    for copy in sent:
        copy.wait_send()


def projected(raw, psi, table, panels, offsets):
    dma = pltpu.SemaphoreType.DMA
    hbm = pl.BlockSpec(memory_space=pltpu.HBM)
    return pl.pallas_call(
        kernel,
        out_shape=jax.ShapeDtypeStruct((COLS, SLAB), F32),
        in_specs=[hbm] * 5,
        out_specs=hbm,
        scratch_shapes=[
            pltpu.VMEM((COLS, SLAB), F32),
            pltpu.VMEM((16, PANEL), F32),
            pltpu.SMEM((2,), jnp.int32),
            pltpu.SMEM((16,), jnp.int32),
            pltpu.VMEM((COLS, SLAB), F32),
            pltpu.VMEM((2, COLS, MINE), F32),
            pltpu.VMEM((2, MINE, BANDS), F32),
            pltpu.VMEM((2, HALF, BANDS), F32),
            pltpu.VMEM((4, 2, COLS, MINE), F32),
            pltpu.VMEM((1024, 2 * MINE), BF16),
            pltpu.VMEM((1024, 2 * MINE), BF16),
            pltpu.VMEM((2 * MINE, BANDS), BF16),
            pltpu.VMEM((2 * MINE, BANDS), BF16),
            pltpu.VMEM((2 * HALF, BANDS), BF16),
            pltpu.VMEM((2 * HALF, BANDS), BF16),
            pltpu.VMEM((32, BANDS), F32),
            pltpu.VMEM((2, 32, BANDS), F32),
            pltpu.VMEM((2, 1024, BANDS), F32),
            pltpu.VMEM((2, 1024, BANDS), F32),
            pltpu.VMEM((4, 2, 2, COLS, L2), F32),
            pltpu.VMEM((4, 2, 2, COLS, L1), F32),
            pltpu.VMEM((2, 512, BANDS), F32),
            pltpu.VMEM((3, 2, 3, 2, 32, BANDS), F32),
            pltpu.VMEM((3, 2, 3, 2, 32, BANDS), F32),
            pltpu.VMEM((3, 2, 2, 32, BANDS), F32),
            pltpu.VMEM((2, 2, COLS, L2), F32),
            pltpu.VMEM((2, COLS, L1), F32),
            pltpu.VMEM((2, 2, 2, COLS, L2), F32),
            pltpu.VMEM((2, 2, COLS, L1), F32),
            pltpu.VMEM((2, COLS, L2), F32),
            pltpu.VMEM((4, 2, COLS, L1), F32),
            dma((12,)), dma((15,)), dma((15,)), dma((5,)), dma((5,)),
            dma((60,)), dma((60,)), dma((24,)), dma((24,)),
        ],
        compiler_params=pltpu.CompilerParams(
            collective_id=0, has_side_effects=True, vmem_limit_bytes=62 * 1024 * 1024
        ),
    )(raw, psi, table, panels, offsets)


def turn_kernel(offsets, value, out):
    offset = offsets[lax.axis_index("ga")]
    for part in (0, 1):
        out[part] = pltpu.roll(value[part], offset, 1)


def turned_back(value, offsets):
    block = pl.BlockSpec((2, 32, SLAB), lambda k: (0, k, 0))
    return pl.pallas_call(
        turn_kernel,
        grid=(COLS // 2 // 32,),
        out_shape=jax.ShapeDtypeStruct((2, COLS // 2, SLAB), F32),
        in_specs=[pl.BlockSpec(memory_space=pltpu.SMEM), block],
        out_specs=block,
        compiler_params=pltpu.CompilerParams(vmem_limit_bytes=62 * 1024 * 1024),
    )(offsets, value)


def per_device(psi, dpsi, band_weight, panel_band, slab_offset):
    raw = jnp.swapaxes(dpsi, 1, 2).reshape(COLS, SLAB)
    result = projected(raw, psi, band_weight.reshape(-1, PANEL), panel_band, slab_offset)
    return jnp.swapaxes(turned_back(result.reshape(2, COLS // 2, SLAB), slab_offset), 1, 2)


def solution(mesh):
    in_specs = (P(None, "ga", "ba"), P(None, "ga", "ba"), P(), P("ba"), P())
    out_specs = P(None, "ga", "ba")
    return jax.shard_map(
        per_device, mesh=mesh, in_specs=in_specs, out_specs=out_specs, check_vma=False
    )
```

```python
import jax
import jax.numpy as jnp
from jax import lax
from jax.experimental import pallas as pl
from jax.experimental.pallas import tpu as pltpu
from jax.sharding import PartitionSpec as P

F32, BF16 = jnp.float32, jnp.bfloat16
PANEL = 128
SLAB = 2048
BANDS = 256
COLS = 128
HALF = 768
BOTH = SLAB - 2 * HALF
MINE = HALF + BOTH
PIECES = (0, 64, 256, 512, 640, HALF)
LAST = PIECES[-2]
L2, L1 = HALF // 2, BOTH // 2
NT = (((1,), (1,)), ((), ()))


def split(value):
    high = value.astype(BF16)
    return high, (value - high.astype(F32)).astype(BF16)


def three(dot, left, right):
    return dot(left[0], right[0]) + (dot(left[0], right[1]) + dot(left[1], right[0]))


def nn(left, right):
    return jnp.dot(left, right, preferred_element_type=F32)


def nt(left, right):
    return lax.dot_general(left, right, NT, preferred_element_type=F32)


def kernel(
    raw_hbm, psi, table_hbm, panels_hbm, offsets_hbm, out,
    raw, table, panels, offsets, at, psi_o, psi_p, a_v, a_hi, a_lo, o_hi, o_lo, p_hi, p_lo, ws, wv, m, w, c2, c1,
    r0, r1, r2, s, rl2, rl1, fin2, fin1, zin, zg,
    local_sem, a_s, a_r, p_s, p_r, g_s, g_r, c_s, c_r,
):
    ga, ba = lax.axis_index("ga"), lax.axis_index("ba")
    x, zhi, core = ga // 4, (ga // 2) % 2, ga % 2
    y, o = ba // 2, ba % 2
    p = 1 - o
    z = zhi * 2 + o
    oc = 1 - core

    def device(x=x, z=z, y=y, core=core):
        return (x * 4 + (z // 2) * 2 + core, y * 2 + z % 2)

    pair = device(z=zhi * 2 + p)
    up, down = device(y=(y + 1) % 4), device(y=(y + 3) % 4)
    other = device(core=oc)
    along_x = [device(x=(x + k) % 4) for k in (1, 2, 3)]
    along_z = [device(z=(z + k) % 4) for k in (1, 2, 3)]

    sent = []

    def send(src, dst, sems, index, to):
        copy = pltpu.make_async_remote_copy(
            src_ref=src, dst_ref=dst, send_sem=sems[0].at[index], recv_sem=sems[1].at[index],
            device_id=to, device_id_type=pl.DeviceIdType.MESH,
        )
        copy.start()
        sent.append(copy)
        return copy

    def half_at(which):
        return pl.multiple_of(which * HALF, HALF)

    barrier = pltpu.get_barrier_semaphore()
    peers = [up, down, other, *along_x, *along_z]
    for peer in peers:
        pl.semaphore_signal(barrier, inc=1, device_id=peer, device_id_type=pl.DeviceIdType.MESH)

    small = [
        pltpu.make_async_copy(offsets_hbm, offsets, local_sem.at[3]),
        pltpu.make_async_copy(table_hbm, table, local_sem.at[4]),
        pltpu.make_async_copy(panels_hbm, panels, local_sem.at[5]),
    ]
    local = [
        pltpu.make_async_copy(raw_hbm, raw, local_sem.at[0]),
        pltpu.make_async_copy(
            psi.at[:, pl.ds(half_at(o), HALF), :], psi_o.at[:, pl.ds(0, HALF), :], local_sem.at[1]
        ),
        pltpu.make_async_copy(
            psi.at[:, pl.ds(2 * HALF, BOTH), :], psi_o.at[:, pl.ds(HALF, BOTH), :], local_sem.at[2]
        ),
    ]
    for copy in small + local:
        copy.start()

    waves = []

    def send_waves(k):
        first, count = PIECES[k], PIECES[k + 1] - PIECES[k]
        waves.append(
            send(
                psi.at[:, pl.ds(pl.multiple_of(p * HALF + first, 64), count), :],
                psi_p.at[:, pl.ds(first, count), :], (p_s, p_r), k, pair,
            )
        )

    pl.semaphore_wait(barrier, len(peers))
    send_waves(0)
    for copy in small:
        copy.wait()
    local[0].wait()

    offset = offsets[ga]
    lane = lax.broadcasted_iota(jnp.int32, (16, 128), 1)

    def align(k, _):
        rows = pl.ds(pl.multiple_of(k * 16, 16), 16)
        tiles = [raw[rows, t * 128 : (t + 1) * 128] for t in range(16)]
        for bit in (10, 9, 8, 7, 6, 5, 4, 3, 2, 1, 0):
            turn = jnp.full((16, 128), (offset >> bit) & 1, jnp.int32) != 0
            if bit >= 7:
                moved = [tiles[(t + (1 << (bit - 7))) % 16] for t in range(16)]
            else:
                rolled = [pltpu.roll(tile, 128 - (1 << bit), 1) for tile in tiles]
                inside = lane < 128 - (1 << bit)
                moved = [jnp.where(inside, rolled[t], rolled[(t + 1) % 16]) for t in range(16)]
            tiles = [jnp.where(turn, new, old) for new, old in zip(moved, tiles)]
        for t, value in enumerate(tiles):
            if t * 128 < 2 * HALF:
                half, first = divmod(t * 128, HALF)
                at[half, rows, first : first + 128] = value
            else:
                first = t * 128 - HALF
                at[0, rows, first : first + 128] = value
                at[1, rows, first : first + 128] = value
        return 0

    lax.fori_loop(0, COLS // 16, align, 0)

    row = lax.broadcasted_iota(jnp.int32, (16, PANEL), 0)
    for k in (0, 1):
        chosen = jnp.where(row == jnp.full((16, PANEL), panels[k], jnp.int32), table[...], 0.0)
        ws[:, k * PANEL : (k + 1) * PANEL] = jnp.broadcast_to(
            jnp.sum(chosen, axis=0, keepdims=True), (32, PANEL)
        )
    wv[o] = ws[...]

    A = (a_s, a_r)
    lanes = (pl.ds(0, MINE // 2), pl.ds(MINE // 2, MINE // 2))
    a_pair = [send(at.at[p, :, l], a_v.at[3, o, :, l], A, i, pair) for i, l in enumerate(lanes)]
    ring = ((0, up, 2), (1, down, 1))

    def pass_on(source, half, base):
        return {
            (way, i): send(source.at[:, lanes[i]], a_v.at[slot, half, :, lanes[i]], A, base + way * 2 + i, to)
            for order in (0, 1) for way, to, slot in ring for i in (way ^ order,)
        }

    def forward(half, base):
        return [
            send(a_v.at[slot, half, :, lanes[way]], a_v.at[0, half, :, lanes[way]], A, base + way, to)
            for way, to, slot in ring
        ]

    near_o = pass_on(at.at[o], o, 2)
    w_pair = send(ws, wv.at[o], A, 14, pair)
    for k in range(1, len(PIECES) - 1):
        send_waves(k)

    def keep_columns(value, rel, half):
        rows = rel * 256 + half * COLS
        top = pl.ds(pl.multiple_of(rows, 64), 64)
        bottom = pl.ds(pl.multiple_of(rows + 64, 64), 64)
        for ref, part in zip((a_hi, a_lo), split(value)):
            ref[top, :MINE] = part[:64]
            ref[bottom, :MINE] = part[64:]
            ref[top, MINE:] = part[64:]
            ref[bottom, MINE:] = -part[:64]

    def keep_waves(ref, high_ref, low_ref, length, first, count):
        for part in (0, 1):
            high, low = split(ref[part, first : first + count, :])
            high_ref[part * length + first : part * length + first + count, :] = high
            low_ref[part * length + first : part * length + first + count, :] = low

    def keep_piece(k):
        waves[k].wait_recv()
        keep_waves(psi_p, p_hi, p_lo, HALF, PIECES[k], PIECES[k + 1] - PIECES[k])

    keep_columns(at[o], 3, o)
    local[1].wait()
    local[2].wait()
    keep_waves(psi_o, o_hi, o_lo, MINE, 0, MINE)
    keep_piece(0)

    for way in (0, 1):
        near_o[way, way].wait_recv()
    far_o = forward(o, 10)
    a_pair[0].wait_recv()
    a_pair[1].wait_recv()
    near_p = pass_on(a_v.at[3, p], p, 6)
    keep_columns(a_v[3, p], 3, p)
    for way, _, slot in ring:
        near_o[way, 1 - way].wait_recv()
        keep_columns(a_v[slot, o], slot, o)
    keep_piece(1)
    for way in (0, 1):
        near_p[way, way].wait_recv()
    far_p = forward(p, 12)
    for copy in far_o:
        copy.wait_recv()
    keep_columns(a_v[0, o], 0, o)
    keep_piece(2)
    for way, _, slot in ring:
        near_p[way, 1 - way].wait_recv()
        keep_columns(a_v[slot, p], slot, p)
    w_pair.wait_recv()

    def own_bands(rel):
        rows = pl.ds(pl.multiple_of(rel * 256, 256), 256)
        m[o, rows, :] = three(nn, (a_hi[rows, :], a_lo[rows, :]), (o_hi[...], o_lo[...]))

    def block_rows(rel):
        return pl.ds(pl.multiple_of(rel * 256, 256), 256)

    def pair_bands(rows, first, last):
        total = None
        for part in (0, 1):
            ks, rs = pl.ds(part * MINE + first, last - first), pl.ds(part * HALF + first, last - first)
            term = three(nn, (a_hi[rows, ks], a_lo[rows, ks]), (p_hi[rs, :], p_lo[rs, :]))
            total = term if total is None else total + term
        return rows, total

    def early(rel, _):
        own_bands(rel)
        rows, total = pair_bands(block_rows(rel), 0, PIECES[3])
        m[p, rows, :] = total
        return 0

    lax.fori_loop(1, 4, early, 0)
    for copy in far_p:
        copy.wait_recv()
    keep_columns(a_v[0, p], 0, p)
    lax.fori_loop(0, 1, early, 0)
    keep_piece(3)

    def later(rel, _):
        rows, total = pair_bands(block_rows(rel), PIECES[3], LAST)
        m[p, rows, :] = m[p, rows, :] + total
        return 0

    lax.fori_loop(0, 4, later, 0)
    keep_piece(4)

    G = (g_s, g_r)
    chunks = ((0, 256), (256, 512), (768, 256))
    flight = {}

    def quarter(n, part, q):
        first, length = chunks[n]
        return pl.ds(
            pl.multiple_of(first + (core * 2 + part) * (length // 4) + q * (length // 16), 8),
            length // 16,
        )

    def core_rows(n, which):
        first, length = chunks[n]
        return pl.ds(pl.multiple_of(first + which * (length // 2), 64), length // 2)

    def landed(n):
        for copy in flight[n]:
            copy.wait_recv()
        flight[n] = []

    def step0(n):
        first, length = chunks[n]
        rows, total = pair_bands(pl.ds(first, length), LAST, HALF)
        m[p, rows, :] = m[p, rows, :] + total
        to = r0.at[:, pl.ds(first // 2, length // 2), :]
        flight[n] = [send(m.at[:, core_rows(n, oc), :], to, G, n * 20, other)]

    def step1(n):
        landed(n)
        first, length = chunks[n]
        rows = core_rows(n, core)
        m[:, rows, :] = m[:, rows, :] + r0[:, first // 2 : (first + length) // 2, :]
        few = pl.ds(0, length // 16)
        for k in (1, 2, 3):
            to_x, to_z = (x + k) % 4, (z + k) % 4
            flight[n] += [
                send(m.at[:, quarter(n, 0, to_x), :], r1.at[n, 0, k - 1, :, few], G, n * 20 + k, along_x[k - 1]),
                send(m.at[:, quarter(n, 1, to_z), :], r1.at[n, 1, k - 1, :, few], G, n * 20 + 3 + k, along_z[k - 1]),
            ]

    def four(mine, ref, n, part):
        few = chunks[n][1] // 16
        return (mine + ref[n, part, 0, :, :few]) + (ref[n, part, 1, :, :few] + ref[n, part, 2, :, :few])

    def step2(n):
        landed(n)
        few = pl.ds(0, chunks[n][1] // 16)
        for part, q in ((0, x), (1, z)):
            s[n, part, :, few, :] = four(m[:, quarter(n, part, q), :], r1, n, part)
        for k in (1, 2, 3):
            flight[n] += [
                send(s.at[n, 0, :, few], r2.at[n, 0, k - 1, :, few], G, n * 20 + 6 + k, along_z[k - 1]),
                send(s.at[n, 1, :, few], r2.at[n, 1, k - 1, :, few], G, n * 20 + 9 + k, along_x[k - 1]),
            ]

    def step3(n):
        landed(n)
        few = chunks[n][1] // 16
        for part, q in ((0, x), (1, z)):
            w[:, quarter(n, part, q), :] = four(s[n, part, :, :few], r2, n, part) * wv[:, :few, :]
        for_x, for_z = w.at[:, quarter(n, 0, x), :], w.at[:, quarter(n, 1, z), :]
        for k in (1, 2, 3):
            flight[n] += [
                send(for_x, for_x, G, n * 20 + 12 + k, along_x[k - 1]),
                send(for_z, for_z, G, n * 20 + 15 + k, along_z[k - 1]),
            ]

    def step4(n):
        landed(n)
        block = w.at[:, core_rows(n, core), :]
        flight[n] = [send(block, block, G, n * 20 + 19, other)]

    C = (c_s, c_r)
    pairs = {}

    def corrections(rel):
        left = []
        for half in (o, p):
            plain = split(w[half, rel * 256 : rel * 256 + 256, :])
            left.append((plain, [
                jnp.concatenate([-v[64:128], v[:64], -v[192:], v[128:192]], axis=0) for v in plain
            ]))
        mine, theirs = left

        def both(l):
            total = None
            for imag in (0, 1):
                rows = pl.ds(imag * MINE + HALF + l * L1, L1)
                term = three(nt, mine[imag], (o_hi[rows, :], o_lo[rows, :]))
                total = term if total is None else total + term
            c1[rel, 0, l] = total[:COLS]
            c1[rel, 1, l] = total[COLS:]

        def alone(l):
            total = None
            for imag in (0, 1):
                rows = pl.ds(imag * MINE + l * L2, L2)
                term = three(nt, mine[imag], (o_hi[rows, :], o_lo[rows, :]))
                total = term if total is None else total + term
                rows = pl.ds(imag * HALF + l * L2, L2)
                total = total + three(nt, theirs[imag], (p_hi[rows, :], p_lo[rows, :]))
            c2[rel, 0, l] = total[:COLS]
            c2[rel, 1, l] = total[COLS:]

        return both, alone

    ways = ((0, 1, up), (1, 2, down))
    relay, final = {}, {}

    def piece(rel, i, l):
        return (c2.at[rel, p, l], c2.at[rel, o, l], c1.at[rel, o, l])[i]

    def summed_over_pair(rel):
        pairs[rel].wait_recv()
        c1[rel, o] = c1[rel, o] + zg[rel]

    def final_slot(way, i, l):
        return fin1.at[way, l] if i == 2 else fin2.at[way, i, l]

    def send_final(way, i, l):
        _, rel, to = ways[way]
        final[way, i, l] = send(
            piece(rel, i, l), final_slot(way, i, l), C, 6 + way * 6 + i * 2 + l, to
        )

    def to_pair(rel):
        pairs[rel] = send(c1.at[rel, p], zg.at[rel], C, 20 + rel, pair)

    def send_relay(i):
        for way, _, to in ways:
            slot = rl1.at[way] if i == 2 else rl2.at[way, i]
            relay[way, i] = send(piece(0, i, way), slot, C, way * 3 + i, to)

    def send_held(way, i):
        relay[way, i].wait_recv()
        held = piece(ways[way][1], i, way)
        held[...] = held[...] + (rl1[way] if i == 2 else rl2[way, i])
        send_final(way, i, way)

    def step5(n):
        landed(n)
        if n == 0:
            both, alone = corrections(0)
            for way, _, to in ways:
                alone(way)
                for i in (0, 1):
                    relay[way, i] = send(piece(0, i, way), rl2.at[way, i], C, way * 3 + i, to)
            both(0)
            both(1)
            to_pair(0)
        elif n == 1:
            summed_over_pair(0)
            send_relay(2)
            for way, rel, _ in ways:
                both, alone = corrections(rel)
                both(0)
                both(1)
                to_pair(rel)
                alone(1 - way)
                send_final(way, 0, 1 - way)
                alone(way)
            for i in (0, 1):
                for way in (0, 1):
                    if i > 0:
                        send_final(way, i, 1 - way)
                for way in (0, 1):
                    send_held(way, i)
        else:
            both, alone = corrections(3)
            both(0)
            both(1)
            to_pair(3)
            for way, rel, _ in ways:
                summed_over_pair(rel)
                send_final(way, 2, 1 - way)
            for way in (0, 1):
                send_held(way, 2)
            alone(0)
            alone(1)

    steps = (step0, step1, step2, step3, step4, step5)
    for t in range(len(steps) + len(chunks) - 1):
        for n in range(len(chunks)):
            if 0 <= t - n < len(steps):
                steps[t - n](n)

    def arrived(i, l):
        final[0, i, l].wait_recv()
        final[1, i, l].wait_recv()
        return piece(3, i, l)[...] + (final_slot(0, i, l)[...] + final_slot(1, i, l)[...])

    across = []
    for l in (0, 1):
        c2[3, p, l] = arrived(0, l)
        across.append(send(c2.at[3, p, l], zin.at[l], C, 18 + l, pair))
    for l in (0, 1):
        lanes = pl.ds(pl.multiple_of(o * HALF + l * L2, 128), L2)
        out[:, lanes] = at[o, :, l * L2 : (l + 1) * L2] - arrived(1, l)
    summed_over_pair(3)
    for l in (0, 1):
        first = HALF + l * L1
        out[:, HALF + first : HALF + first + L1] = at[o, :, first : first + L1] - arrived(2, l)
    for l in (0, 1):
        across[l].wait_recv()
        lanes = pl.ds(pl.multiple_of(p * HALF + l * L2, 128), L2)
        out[:, lanes] = at[p, :, l * L2 : (l + 1) * L2] - zin[l]

    for copy in sent:
        copy.wait_send()


def projected(raw, psi, table, panels, offsets):
    dma = pltpu.SemaphoreType.DMA
    vmem, hbm = pl.BlockSpec(memory_space=pltpu.VMEM), pl.BlockSpec(memory_space=pltpu.HBM)
    return pl.pallas_call(
        kernel,
        out_shape=jax.ShapeDtypeStruct((COLS, SLAB), F32),
        in_specs=[hbm] * 5,
        out_specs=vmem,
        scratch_shapes=[
            pltpu.VMEM((COLS, SLAB), F32),
            pltpu.VMEM((16, PANEL), F32),
            pltpu.SMEM((2,), jnp.int32),
            pltpu.SMEM((16,), jnp.int32),
            pltpu.VMEM((2, COLS, MINE), F32),
            pltpu.VMEM((2, MINE, BANDS), F32),
            pltpu.VMEM((2, HALF, BANDS), F32),
            pltpu.VMEM((4, 2, COLS, MINE), F32),
            pltpu.VMEM((1024, 2 * MINE), BF16),
            pltpu.VMEM((1024, 2 * MINE), BF16),
            pltpu.VMEM((2 * MINE, BANDS), BF16),
            pltpu.VMEM((2 * MINE, BANDS), BF16),
            pltpu.VMEM((2 * HALF, BANDS), BF16),
            pltpu.VMEM((2 * HALF, BANDS), BF16),
            pltpu.VMEM((32, BANDS), F32),
            pltpu.VMEM((2, 32, BANDS), F32),
            pltpu.VMEM((2, 1024, BANDS), F32),
            pltpu.VMEM((2, 1024, BANDS), F32),
            pltpu.VMEM((4, 2, 2, COLS, L2), F32),
            pltpu.VMEM((4, 2, 2, COLS, L1), F32),
            pltpu.VMEM((2, 512, BANDS), F32),
            pltpu.VMEM((3, 2, 3, 2, 32, BANDS), F32),
            pltpu.VMEM((3, 2, 3, 2, 32, BANDS), F32),
            pltpu.VMEM((3, 2, 2, 32, BANDS), F32),
            pltpu.VMEM((2, 2, COLS, L2), F32),
            pltpu.VMEM((2, COLS, L1), F32),
            pltpu.VMEM((2, 2, 2, COLS, L2), F32),
            pltpu.VMEM((2, 2, COLS, L1), F32),
            pltpu.VMEM((2, COLS, L2), F32),
            pltpu.VMEM((4, 2, COLS, L1), F32),
            dma((6,)), dma((15,)), dma((15,)), dma((5,)), dma((5,)),
            dma((60,)), dma((60,)), dma((24,)), dma((24,)),
        ],
        compiler_params=pltpu.CompilerParams(
            collective_id=0, has_side_effects=True, vmem_limit_bytes=62 * 1024 * 1024
        ),
    )(raw, psi, table, panels, offsets)


def turn_kernel(offsets, value, out):
    offset = offsets[lax.axis_index("ga")]
    for part in (0, 1):
        out[part] = pltpu.roll(value[part], offset, 1)


def turned_back(value, offsets):
    block = pl.BlockSpec((2, 32, SLAB), lambda k: (0, k, 0))
    return pl.pallas_call(
        turn_kernel,
        grid=(COLS // 2 // 32,),
        out_shape=jax.ShapeDtypeStruct((2, COLS // 2, SLAB), F32),
        in_specs=[pl.BlockSpec(memory_space=pltpu.SMEM), block],
        out_specs=block,
        compiler_params=pltpu.CompilerParams(vmem_limit_bytes=62 * 1024 * 1024),
    )(offsets, value)


def per_device(psi, dpsi, band_weight, panel_band, slab_offset):
    raw = jnp.swapaxes(dpsi, 1, 2).reshape(COLS, SLAB)
    result = projected(raw, psi, band_weight.reshape(-1, PANEL), panel_band, slab_offset)
    return jnp.swapaxes(turned_back(result.reshape(2, COLS // 2, SLAB), slab_offset), 1, 2)


def solution(mesh):
    in_specs = (P(None, "ga", "ba"), P(None, "ga", "ba"), P(), P("ba"), P())
    out_specs = P(None, "ga", "ba")
    return jax.shard_map(
        per_device, mesh=mesh, in_specs=in_specs, out_specs=out_specs, check_vma=False
    )
```

```python
import jax
import jax.numpy as jnp
from jax import lax
from jax.experimental import pallas as pl
from jax.experimental.pallas import tpu as pltpu
from jax.sharding import PartitionSpec as P

F32, BF16 = jnp.float32, jnp.bfloat16
PANEL = 128
SLAB = 2048
BANDS = 256
COLS = 128
HALF = 768
BOTH = SLAB - 2 * HALF
MINE = HALF + BOTH
PIECES = (0, 64, 256, 512, 640, HALF)
LAST = PIECES[-2]
L2, L1 = HALF // 2, BOTH // 2
NT = (((1,), (1,)), ((), ()))


def split(value):
    high = value.astype(BF16)
    return high, (value - high.astype(F32)).astype(BF16)


def three(dot, left, right):
    return dot(left[0], right[0]) + (dot(left[0], right[1]) + dot(left[1], right[0]))


def nn(left, right):
    return jnp.dot(left, right, preferred_element_type=F32)


def nt(left, right):
    return lax.dot_general(left, right, NT, preferred_element_type=F32)


def kernel(
    raw_hbm, psi, table_hbm, panels_hbm, offsets_hbm, out,
    raw, table, panels, offsets, out_v, at, psi_o, psi_p, a_v, a_hi, a_lo, o_hi, o_lo, p_hi, p_lo, ws, wv, m, w, c2, c1,
    r0, r1, r2, s, rl2, rl1, fin2, fin1, zin, zg,
    local_sem, a_s, a_r, p_s, p_r, g_s, g_r, c_s, c_r,
):
    ga, ba = lax.axis_index("ga"), lax.axis_index("ba")
    x, zhi, core = ga // 4, (ga // 2) % 2, ga % 2
    y, o = ba // 2, ba % 2
    p = 1 - o
    z = zhi * 2 + o
    oc = 1 - core

    def device(x=x, z=z, y=y, core=core):
        return (x * 4 + (z // 2) * 2 + core, y * 2 + z % 2)

    pair = device(z=zhi * 2 + p)
    up, down = device(y=(y + 1) % 4), device(y=(y + 3) % 4)
    other = device(core=oc)
    along_x = [device(x=(x + k) % 4) for k in (1, 2, 3)]
    along_z = [device(z=(z + k) % 4) for k in (1, 2, 3)]

    sent = []

    def send(src, dst, sems, index, to):
        copy = pltpu.make_async_remote_copy(
            src_ref=src, dst_ref=dst, send_sem=sems[0].at[index], recv_sem=sems[1].at[index],
            device_id=to, device_id_type=pl.DeviceIdType.MESH,
        )
        copy.start()
        sent.append(copy)
        return copy

    def half_at(which):
        return pl.multiple_of(which * HALF, HALF)

    barrier = pltpu.get_barrier_semaphore()
    peers = [up, down, other, *along_x, *along_z]
    for peer in peers:
        pl.semaphore_signal(barrier, inc=1, device_id=peer, device_id_type=pl.DeviceIdType.MESH)

    small = [
        pltpu.make_async_copy(offsets_hbm, offsets, local_sem.at[3]),
        pltpu.make_async_copy(table_hbm, table, local_sem.at[4]),
        pltpu.make_async_copy(panels_hbm, panels, local_sem.at[5]),
    ]
    local = [
        pltpu.make_async_copy(raw_hbm, raw, local_sem.at[0]),
        pltpu.make_async_copy(
            psi.at[:, pl.ds(half_at(o), HALF), :], psi_o.at[:, pl.ds(0, HALF), :], local_sem.at[1]
        ),
        pltpu.make_async_copy(
            psi.at[:, pl.ds(2 * HALF, BOTH), :], psi_o.at[:, pl.ds(HALF, BOTH), :], local_sem.at[2]
        ),
    ]
    for copy in small + local:
        copy.start()

    waves = []

    def send_waves(k):
        first, count = PIECES[k], PIECES[k + 1] - PIECES[k]
        waves.append(
            send(
                psi.at[:, pl.ds(pl.multiple_of(p * HALF + first, 64), count), :],
                psi_p.at[:, pl.ds(first, count), :], (p_s, p_r), k, pair,
            )
        )

    pl.semaphore_wait(barrier, len(peers))
    send_waves(0)
    for copy in small:
        copy.wait()
    local[0].wait()

    offset = offsets[ga]
    lane = lax.broadcasted_iota(jnp.int32, (16, 128), 1)

    def align(k, _):
        rows = pl.ds(pl.multiple_of(k * 16, 16), 16)
        tiles = [raw[rows, t * 128 : (t + 1) * 128] for t in range(16)]
        for bit in (10, 9, 8, 7, 6, 5, 4, 3, 2, 1, 0):
            turn = jnp.full((16, 128), (offset >> bit) & 1, jnp.int32) != 0
            if bit >= 7:
                moved = [tiles[(t + (1 << (bit - 7))) % 16] for t in range(16)]
            else:
                rolled = [pltpu.roll(tile, 128 - (1 << bit), 1) for tile in tiles]
                inside = lane < 128 - (1 << bit)
                moved = [jnp.where(inside, rolled[t], rolled[(t + 1) % 16]) for t in range(16)]
            tiles = [jnp.where(turn, new, old) for new, old in zip(moved, tiles)]
        for t, value in enumerate(tiles):
            if t * 128 < 2 * HALF:
                half, first = divmod(t * 128, HALF)
                at[half, rows, first : first + 128] = value
            else:
                first = t * 128 - HALF
                at[0, rows, first : first + 128] = value
                at[1, rows, first : first + 128] = value
        return 0

    lax.fori_loop(0, COLS // 16, align, 0)

    row = lax.broadcasted_iota(jnp.int32, (16, PANEL), 0)
    for k in (0, 1):
        chosen = jnp.where(row == jnp.full((16, PANEL), panels[k], jnp.int32), table[...], 0.0)
        ws[:, k * PANEL : (k + 1) * PANEL] = jnp.broadcast_to(
            jnp.sum(chosen, axis=0, keepdims=True), (32, PANEL)
        )
    wv[o] = ws[...]

    A = (a_s, a_r)
    lanes = (pl.ds(0, MINE // 2), pl.ds(MINE // 2, MINE // 2))
    a_pair = [send(at.at[p, :, l], a_v.at[3, o, :, l], A, i, pair) for i, l in enumerate(lanes)]
    ring = ((0, up, 2), (1, down, 1))

    def pass_on(source, half, base):
        return {
            (way, i): send(source.at[:, lanes[i]], a_v.at[slot, half, :, lanes[i]], A, base + way * 2 + i, to)
            for order in (0, 1) for way, to, slot in ring for i in (way ^ order,)
        }

    def forward(half, base):
        return [
            send(a_v.at[slot, half, :, lanes[way]], a_v.at[0, half, :, lanes[way]], A, base + way, to)
            for way, to, slot in ring
        ]

    near_o = pass_on(at.at[o], o, 2)
    w_pair = send(ws, wv.at[o], A, 14, pair)
    for k in range(1, len(PIECES) - 1):
        send_waves(k)

    def keep_columns(value, rel, half):
        rows = rel * 256 + half * COLS
        top = pl.ds(pl.multiple_of(rows, 64), 64)
        bottom = pl.ds(pl.multiple_of(rows + 64, 64), 64)
        for ref, part in zip((a_hi, a_lo), split(value)):
            ref[top, :MINE] = part[:64]
            ref[bottom, :MINE] = part[64:]
            ref[top, MINE:] = part[64:]
            ref[bottom, MINE:] = -part[:64]

    def keep_waves(ref, high_ref, low_ref, length, first, count):
        for part in (0, 1):
            high, low = split(ref[part, first : first + count, :])
            high_ref[part * length + first : part * length + first + count, :] = high
            low_ref[part * length + first : part * length + first + count, :] = low

    def keep_piece(k):
        waves[k].wait_recv()
        keep_waves(psi_p, p_hi, p_lo, HALF, PIECES[k], PIECES[k + 1] - PIECES[k])

    keep_columns(at[o], 3, o)
    local[1].wait()
    local[2].wait()
    keep_waves(psi_o, o_hi, o_lo, MINE, 0, MINE)
    keep_piece(0)

    for way in (0, 1):
        near_o[way, way].wait_recv()
    far_o = forward(o, 10)
    a_pair[0].wait_recv()
    a_pair[1].wait_recv()
    near_p = pass_on(a_v.at[3, p], p, 6)
    keep_columns(a_v[3, p], 3, p)
    for way, _, slot in ring:
        near_o[way, 1 - way].wait_recv()
        keep_columns(a_v[slot, o], slot, o)
    keep_piece(1)
    for way in (0, 1):
        near_p[way, way].wait_recv()
    far_p = forward(p, 12)
    for copy in far_o:
        copy.wait_recv()
    keep_columns(a_v[0, o], 0, o)
    keep_piece(2)
    for way, _, slot in ring:
        near_p[way, 1 - way].wait_recv()
        keep_columns(a_v[slot, p], slot, p)
    w_pair.wait_recv()

    def own_bands(rel):
        rows = pl.ds(pl.multiple_of(rel * 256, 256), 256)
        m[o, rows, :] = three(nn, (a_hi[rows, :], a_lo[rows, :]), (o_hi[...], o_lo[...]))

    def block_rows(rel):
        return pl.ds(pl.multiple_of(rel * 256, 256), 256)

    def pair_bands(rows, first, last):
        total = None
        for part in (0, 1):
            ks, rs = pl.ds(part * MINE + first, last - first), pl.ds(part * HALF + first, last - first)
            term = three(nn, (a_hi[rows, ks], a_lo[rows, ks]), (p_hi[rs, :], p_lo[rs, :]))
            total = term if total is None else total + term
        return rows, total

    def early(rel, _):
        own_bands(rel)
        rows, total = pair_bands(block_rows(rel), 0, PIECES[3])
        m[p, rows, :] = total
        return 0

    lax.fori_loop(1, 4, early, 0)
    for copy in far_p:
        copy.wait_recv()
    keep_columns(a_v[0, p], 0, p)
    lax.fori_loop(0, 1, early, 0)
    keep_piece(3)

    def later(rel, _):
        rows, total = pair_bands(block_rows(rel), PIECES[3], LAST)
        m[p, rows, :] = m[p, rows, :] + total
        return 0

    lax.fori_loop(0, 4, later, 0)
    keep_piece(4)

    G = (g_s, g_r)
    chunks = ((0, 256), (256, 512), (768, 256))
    flight = {}

    def quarter(n, part, q):
        first, length = chunks[n]
        return pl.ds(
            pl.multiple_of(first + (core * 2 + part) * (length // 4) + q * (length // 16), 8),
            length // 16,
        )

    def core_rows(n, which):
        first, length = chunks[n]
        return pl.ds(pl.multiple_of(first + which * (length // 2), 64), length // 2)

    def landed(n):
        for copy in flight[n]:
            copy.wait_recv()
        flight[n] = []

    def step0(n):
        first, length = chunks[n]
        rows, total = pair_bands(pl.ds(first, length), LAST, HALF)
        m[p, rows, :] = m[p, rows, :] + total
        to = r0.at[:, pl.ds(first // 2, length // 2), :]
        flight[n] = [send(m.at[:, core_rows(n, oc), :], to, G, n * 20, other)]

    def step1(n):
        landed(n)
        first, length = chunks[n]
        rows = core_rows(n, core)
        m[:, rows, :] = m[:, rows, :] + r0[:, first // 2 : (first + length) // 2, :]
        few = pl.ds(0, length // 16)
        for k in (1, 2, 3):
            to_x, to_z = (x + k) % 4, (z + k) % 4
            flight[n] += [
                send(m.at[:, quarter(n, 0, to_x), :], r1.at[n, 0, k - 1, :, few], G, n * 20 + k, along_x[k - 1]),
                send(m.at[:, quarter(n, 1, to_z), :], r1.at[n, 1, k - 1, :, few], G, n * 20 + 3 + k, along_z[k - 1]),
            ]

    def four(mine, ref, n, part):
        few = chunks[n][1] // 16
        return (mine + ref[n, part, 0, :, :few]) + (ref[n, part, 1, :, :few] + ref[n, part, 2, :, :few])

    def step2(n):
        landed(n)
        few = pl.ds(0, chunks[n][1] // 16)
        for part, q in ((0, x), (1, z)):
            s[n, part, :, few, :] = four(m[:, quarter(n, part, q), :], r1, n, part)
        for k in (1, 2, 3):
            flight[n] += [
                send(s.at[n, 0, :, few], r2.at[n, 0, k - 1, :, few], G, n * 20 + 6 + k, along_z[k - 1]),
                send(s.at[n, 1, :, few], r2.at[n, 1, k - 1, :, few], G, n * 20 + 9 + k, along_x[k - 1]),
            ]

    def step3(n):
        landed(n)
        few = chunks[n][1] // 16
        for part, q in ((0, x), (1, z)):
            w[:, quarter(n, part, q), :] = four(s[n, part, :, :few], r2, n, part) * wv[:, :few, :]
        for_x, for_z = w.at[:, quarter(n, 0, x), :], w.at[:, quarter(n, 1, z), :]
        for k in (1, 2, 3):
            flight[n] += [
                send(for_x, for_x, G, n * 20 + 12 + k, along_x[k - 1]),
                send(for_z, for_z, G, n * 20 + 15 + k, along_z[k - 1]),
            ]

    def step4(n):
        landed(n)
        block = w.at[:, core_rows(n, core), :]
        flight[n] = [send(block, block, G, n * 20 + 19, other)]

    C = (c_s, c_r)
    pairs = {}

    def corrections(rel):
        left = []
        for half in (o, p):
            plain = split(w[half, rel * 256 : rel * 256 + 256, :])
            left.append((plain, [
                jnp.concatenate([-v[64:128], v[:64], -v[192:], v[128:192]], axis=0) for v in plain
            ]))
        mine, theirs = left

        def both(l):
            total = None
            for imag in (0, 1):
                rows = pl.ds(imag * MINE + HALF + l * L1, L1)
                term = three(nt, mine[imag], (o_hi[rows, :], o_lo[rows, :]))
                total = term if total is None else total + term
            c1[rel, 0, l] = total[:COLS]
            c1[rel, 1, l] = total[COLS:]
            copy = send(c1.at[rel, p, l], zg.at[rel, l], C, 20 + rel * 2 + l, pair)
            pairs.setdefault(rel, []).append(copy)

        def alone(l):
            total = None
            for imag in (0, 1):
                rows = pl.ds(imag * MINE + l * L2, L2)
                term = three(nt, mine[imag], (o_hi[rows, :], o_lo[rows, :]))
                total = term if total is None else total + term
                rows = pl.ds(imag * HALF + l * L2, L2)
                total = total + three(nt, theirs[imag], (p_hi[rows, :], p_lo[rows, :]))
            c2[rel, 0, l] = total[:COLS]
            c2[rel, 1, l] = total[COLS:]

        return both, alone

    ways = ((0, 1, up), (1, 2, down))
    relay, final = {}, {}

    def piece(rel, i, l):
        return (c2.at[rel, p, l], c2.at[rel, o, l], c1.at[rel, o, l])[i]

    def summed_over_pair(rel):
        for copy in pairs[rel]:
            copy.wait_recv()
        c1[rel, o] = c1[rel, o] + zg[rel]

    def final_slot(way, i, l):
        return fin1.at[way, l] if i == 2 else fin2.at[way, i, l]

    def send_final(way, i, l):
        _, rel, to = ways[way]
        final[way, i, l] = send(
            piece(rel, i, l), final_slot(way, i, l), C, 6 + way * 6 + i * 2 + l, to
        )

    def send_relay(i):
        for way, _, to in ways:
            slot = rl1.at[way] if i == 2 else rl2.at[way, i]
            relay[way, i] = send(piece(0, i, way), slot, C, way * 3 + i, to)

    def send_held(way, i):
        relay[way, i].wait_recv()
        held = piece(ways[way][1], i, way)
        held[...] = held[...] + (rl1[way] if i == 2 else rl2[way, i])
        send_final(way, i, way)

    def step5(n):
        landed(n)
        if n == 0:
            both, alone = corrections(0)
            for way, _, to in ways:
                alone(way)
                for i in (0, 1):
                    relay[way, i] = send(piece(0, i, way), rl2.at[way, i], C, way * 3 + i, to)
            both(0)
            both(1)
        elif n == 1:
            for way, rel, _ in ways:
                both, alone = corrections(rel)
                both(0)
                both(1)
                if way == 0:
                    summed_over_pair(0)
                    send_relay(2)
                alone(1 - way)
                send_final(way, 0, 1 - way)
                alone(way)
            for i in (0, 1):
                for way in (0, 1):
                    if i > 0:
                        send_final(way, i, 1 - way)
                for way in (0, 1):
                    send_held(way, i)
        else:
            both, alone = corrections(3)
            both(0)
            both(1)
            for way, rel, _ in ways:
                summed_over_pair(rel)
                send_final(way, 2, 1 - way)
            for way in (0, 1):
                send_held(way, 2)
            alone(0)
            alone(1)

    steps = (step0, step1, step2, step3, step4, step5)
    for t in range(len(steps) + len(chunks) - 1):
        for n in range(len(chunks)):
            if 0 <= t - n < len(steps):
                steps[t - n](n)

    def arrived(i, l):
        final[0, i, l].wait_recv()
        final[1, i, l].wait_recv()
        return piece(3, i, l)[...] + (final_slot(0, i, l)[...] + final_slot(1, i, l)[...])

    across, written = [], []

    def write(first, length, value):
        lanes = pl.ds(first, length)
        out_v[:, lanes] = value
        copy = pltpu.make_async_copy(out_v.at[:, lanes], out.at[:, lanes], local_sem.at[6 + len(written)])
        copy.start()
        written.append(copy)

    for l in (0, 1):
        c2[3, p, l] = arrived(0, l)
        across.append(send(c2.at[3, p, l], zin.at[l], C, 18 + l, pair))
    for l in (0, 1):
        value = at[o, :, l * L2 : (l + 1) * L2] - arrived(1, l)
        write(pl.multiple_of(o * HALF + l * L2, 128), L2, value)
    summed_over_pair(3)
    for l in (0, 1):
        first = HALF + l * L1
        value = at[o, :, first : first + L1] - arrived(2, l)
        write(HALF + first, L1, value)
    for l in (0, 1):
        across[l].wait_recv()
        value = at[p, :, l * L2 : (l + 1) * L2] - zin[l]
        write(pl.multiple_of(p * HALF + l * L2, 128), L2, value)

    for copy in written:
        copy.wait()
    for copy in sent:
        copy.wait_send()


def projected(raw, psi, table, panels, offsets):
    dma = pltpu.SemaphoreType.DMA
    hbm = pl.BlockSpec(memory_space=pltpu.HBM)
    return pl.pallas_call(
        kernel,
        out_shape=jax.ShapeDtypeStruct((COLS, SLAB), F32),
        in_specs=[hbm] * 5,
        out_specs=hbm,
        scratch_shapes=[
            pltpu.VMEM((COLS, SLAB), F32),
            pltpu.VMEM((16, PANEL), F32),
            pltpu.SMEM((2,), jnp.int32),
            pltpu.SMEM((16,), jnp.int32),
            pltpu.VMEM((COLS, SLAB), F32),
            pltpu.VMEM((2, COLS, MINE), F32),
            pltpu.VMEM((2, MINE, BANDS), F32),
            pltpu.VMEM((2, HALF, BANDS), F32),
            pltpu.VMEM((4, 2, COLS, MINE), F32),
            pltpu.VMEM((1024, 2 * MINE), BF16),
            pltpu.VMEM((1024, 2 * MINE), BF16),
            pltpu.VMEM((2 * MINE, BANDS), BF16),
            pltpu.VMEM((2 * MINE, BANDS), BF16),
            pltpu.VMEM((2 * HALF, BANDS), BF16),
            pltpu.VMEM((2 * HALF, BANDS), BF16),
            pltpu.VMEM((32, BANDS), F32),
            pltpu.VMEM((2, 32, BANDS), F32),
            pltpu.VMEM((2, 1024, BANDS), F32),
            pltpu.VMEM((2, 1024, BANDS), F32),
            pltpu.VMEM((4, 2, 2, COLS, L2), F32),
            pltpu.VMEM((4, 2, 2, COLS, L1), F32),
            pltpu.VMEM((2, 512, BANDS), F32),
            pltpu.VMEM((3, 2, 3, 2, 32, BANDS), F32),
            pltpu.VMEM((3, 2, 3, 2, 32, BANDS), F32),
            pltpu.VMEM((3, 2, 2, 32, BANDS), F32),
            pltpu.VMEM((2, 2, COLS, L2), F32),
            pltpu.VMEM((2, COLS, L1), F32),
            pltpu.VMEM((2, 2, 2, COLS, L2), F32),
            pltpu.VMEM((2, 2, COLS, L1), F32),
            pltpu.VMEM((2, COLS, L2), F32),
            pltpu.VMEM((4, 2, COLS, L1), F32),
            dma((12,)), dma((15,)), dma((15,)), dma((5,)), dma((5,)),
            dma((60,)), dma((60,)), dma((28,)), dma((28,)),
        ],
        compiler_params=pltpu.CompilerParams(
            collective_id=0, has_side_effects=True, vmem_limit_bytes=62 * 1024 * 1024
        ),
    )(raw, psi, table, panels, offsets)


def turn_kernel(offsets, value, out):
    offset = offsets[lax.axis_index("ga")]
    for part in (0, 1):
        out[part] = pltpu.roll(value[part], offset, 1)


def turned_back(value, offsets):
    block = pl.BlockSpec((2, 32, SLAB), lambda k: (0, k, 0))
    return pl.pallas_call(
        turn_kernel,
        grid=(COLS // 2 // 32,),
        out_shape=jax.ShapeDtypeStruct((2, COLS // 2, SLAB), F32),
        in_specs=[pl.BlockSpec(memory_space=pltpu.SMEM), block],
        out_specs=block,
        compiler_params=pltpu.CompilerParams(vmem_limit_bytes=62 * 1024 * 1024),
    )(offsets, value)


def per_device(psi, dpsi, band_weight, panel_band, slab_offset):
    raw = jnp.swapaxes(dpsi, 1, 2).reshape(COLS, SLAB)
    result = projected(raw, psi, band_weight.reshape(-1, PANEL), panel_band, slab_offset)
    return jnp.swapaxes(turned_back(result.reshape(2, COLS // 2, SLAB), slab_offset), 1, 2)


def solution(mesh):
    in_specs = (P(None, "ga", "ba"), P(None, "ga", "ba"), P(), P("ba"), P())
    out_specs = P(None, "ga", "ba")
    return jax.shard_map(
        per_device, mesh=mesh, in_specs=in_specs, out_specs=out_specs, check_vma=False
    )
```
